256 devices in a mesh: groups: 2 (over y), gx: 128 (over z, x, core).
Axes of the slice: x: 4, y: 2, z: 16, core: 2. Of those that a mesh axis runs over, the one named last changes fastest.
The devices are a block of a 4x16x16 slice.
Arguments:
- pressure: float32 [7, 2048, 128, 128], P(None, ('groups', 'gx')), parts along dimension 1, may hold values from -6 to 6
- adjoint: float32 [7, 2048, 128, 128], P(None, ('groups', 'gx')), parts along dimension 1, may hold values from -6 to 6
- permeability: float32 [3, 2048, 128, 128], P(None, ('groups', 'gx')), parts along dimension 1, may hold values from 0.02 to 40, as said below
- active: int32 [2048, 128, 128], P(('groups', 'gx')), parts along dimension 0, may hold values 0 or 1
- fault_codes: int32 [3, 2048, 128, 128], P(None, ('groups', 'gx')), parts along dimension 1, may hold values from 0 to 3
Outputs:
- gradient: float32 [3, 2048, 128, 128], P(None, ('groups', 'gx')), parts along dimension 1
The draws below stay inside these ranges and needn't reach their ends.
There are 2 independent parts, one for each index of `groups`. The reference program is written for one: setup_inputs(seed, part) draws one part's arguments, and reference() takes and returns one part's arrays. A program takes and returns all parts, laid end to end along the dimension named above; each array names one. Nothing has to cross between parts.
Inputs may be any that keep to these rules, and one draw needn't show every extreme that they name: `permeability`: Positive.
All inputs are finite; a program needn't handle non-finite values. No bound on the sum of `active` on one device may be relied on, other than what follows from the above.
Results may differ from the reference program's by a relative error of at most 0.0003.
Values sent between devices are 32-bit elements; how exact they have to be, the bound alone decides.
A program may use at most 64 MiB of HBM per device.

```python
import jax
import jax.numpy as jnp
from jax import lax

NT = 7
NY = 128
NZ = 128
NX = 1024


def draw_permeability(key, part):
    shape = (3, NX, NY, NZ)
    position = jnp.arange(NX, dtype=jnp.float32) / NX
    rough = jnp.clip(0.7 * jax.random.normal(key, shape, jnp.float32), -2.1, 2.1)
    trend = 1.0 + 2.0 * position
    aniso = jnp.array([1.0, 1.0, 0.2], jnp.float32).reshape(3, 1, 1, 1)
    return (aniso * jnp.exp(rough) * trend[None, :, None, None]).astype(jnp.float32)


def plant(values, stream_key, least, high):
    longest = values.shape.index(max(values.shape))
    spots = []
    for shift in (0, 1):
        where = [jax.random.randint(jax.random.fold_in(stream_key, axis), (), 0, length) for axis, length in enumerate(values.shape)]
        where[longest] = (where[longest] + shift) % values.shape[longest]
        spots.append(tuple(where))
    return values.at[spots[0]].set(least).at[spots[1]].set(high)


def steps_of(rng, dims, split, least, high):
    level, own = 1.0, jax.random.fold_in(rng, 6)
    for axis_at, parts in split:
        steps = jnp.exp(jax.random.uniform(jax.random.fold_in(own, axis_at), (parts,), jnp.float32, least / len(split), high / len(split)))
        level = level * jnp.repeat(steps, dims[axis_at] // parts).reshape([-1 if axis == axis_at else 1 for axis in range(len(dims))])
    return level


def scatter_about(key, extent, width, reach, split=(), kind=jnp.bfloat16):
    drawn = jax.random.normal(key, extent, jnp.float32) * width
    if len(split) > 0:
        drawn = steps_of(key, extent, split, -0.22, 0.18) * drawn
    return jnp.clip(drawn, min=-reach, max=reach).astype(kind)


def setup_inputs(seed: int = 0, part: int = 0) -> dict:
    splits = jax.random.split(jax.random.key(seed), 6)
    part_splits = jax.random.split(jax.random.fold_in(splits[5], part), 6)
    return {
        "pressure": scatter_about(part_splits[0], (NT, NX, NY, NZ), 1.0, 6.0, ((1, 128),), jnp.float32),
        "adjoint": scatter_about(part_splits[1], (NT, NX, NY, NZ), 1.0, 6.0, ((1, 128),), jnp.float32),
        "permeability": draw_permeability(jax.random.fold_in(jax.random.fold_in(splits[5], part), 71), part),
        "active": plant((jax.random.randint(part_splits[3], (NX, NY, NZ), 0, 10) < 9).astype(jnp.int32), jax.random.fold_in(part_splits[3], 1), 0, 1),
        "fault_codes": plant(jax.random.randint(part_splits[4], (3, NX, NY, NZ), 0, 4), jax.random.fold_in(part_splits[4], 1), 0, 3).astype(jnp.int32),
    }


epsilon = 1e-06

def multiplier(codes):
    return jnp.where(codes == 0, 1.0, jnp.where(codes == 1, 0.6, jnp.where(codes == 2, 0.25, 0.05))).astype(jnp.float32)

def pair_terms(lower_pres, upper_pres, lower_adj, upper_adj, lower_perm, upper_perm, factor):
    products = lax.optimization_barrier(jnp.sum((lower_adj - upper_adj) * (lower_pres - upper_pres), axis=0))
    summed = lower_perm + upper_perm
    scaled = 2.0 * factor * products / (summed * summed)
    return (scaled * upper_perm * upper_perm, scaled * lower_perm * lower_perm)

def cut(values, start, stop, along):
    return lax.slice_in_dim(values, start, stop, axis=along)

def direction_grad(pressure, adjoint, perm_dir, opened, codes, along):
    count = opened.shape[along]
    factor = multiplier(cut(codes, 0, count - 1, along)) * cut(opened, 0, count - 1, along) * cut(opened, 1, count, along)
    to_lower, to_upper = pair_terms(cut(pressure, 0, count - 1, along + 1), cut(pressure, 1, count, along + 1), cut(adjoint, 0, count - 1, along + 1), cut(adjoint, 1, count, along + 1), cut(perm_dir, 0, count - 1, along), cut(perm_dir, 1, count, along), factor)
    widths_lower = [(0, 0), (0, 0), (0, 0)]
    widths_upper = [(0, 0), (0, 0), (0, 0)]
    widths_lower[along] = (0, 1)
    widths_upper[along] = (1, 0)
    return jnp.pad(to_lower, widths_lower) + jnp.pad(to_upper, widths_upper)

def reference(pressure, adjoint, permeability, active, fault_codes):
    opened = active.astype(jnp.float32)
    logs = []
    for direction in range(3):
        grad = direction_grad(pressure, adjoint, permeability[direction], opened, fault_codes[direction], direction)
        logs.append(permeability[direction] * grad)
    stacked = jnp.stack(logs)
    total = jnp.sum(stacked * stacked)
    root_mean = jnp.sqrt(total / (3 * NX * NY * NZ) + epsilon)
    return stacked / root_mean
```

```python
import functools

import jax
import jax.numpy as jnp
from jax import lax
from jax.experimental import pallas as pl
from jax.experimental.pallas import tpu as pltpu
from jax.sharding import PartitionSpec as P

MESH = pl.DeviceIdType.MESH
F32 = jnp.float32

epsilon = 1e-06

PLANE = 8
BLOCK = 32


def multiplier(codes):
    return jnp.where(codes == 0, 1.0, jnp.where(codes == 1, 0.6, jnp.where(codes == 2, 0.25, 0.05)))


def face(products, factor, lower_perm, upper_perm):
    inverse = 1.0 / (lower_perm + upper_perm)
    weight = (2.0 * factor) * products
    upper = upper_perm * inverse
    lower = lower_perm * inverse
    return weight * upper * upper, weight * lower * lower


def kernel(
    steps, layers, rows, n,
    pres_hbm, adj_hbm, perm_hbm, act_hbm, code_hbm,
    log_ref, inv_ref,
    pres, adj, perm, act, code,
    to_up_x, to_up_y,
    above_pres, above_adj, above_perm, above_act, above_log,
    below_pres, below_adj, below_perm, below_factor, below_log,
    stage_factor, stage_low, stage_high, stage_ra, stage_rb, got_ra, got_rb,
    stage_z, buf_z, stage_p, buf_p,
    load_sem, send_up, recv_up, send_down, recv_down,
    send_z, recv_z, send_p, recv_p, hand,
):
    half = rows // 2
    cells = layers * rows
    top = cells - rows
    planes = n // PLANE
    me = lax.axis_index("gx")
    my_z = me // PLANE
    my_p = lax.rem(me, PLANE)
    up = lax.rem(me + 1, n)
    down = lax.rem(me + n - 1, n)

    def z_peer(by):
        return lax.rem(my_z + planes + by, planes) * PLANE + my_p

    def p_peer(by):
        return my_z * PLANE + lax.rem(my_p + by, PLANE)

    def signal(sem, device):
        pl.semaphore_signal(sem, inc=1, device_id={"gx": device}, device_id_type=MESH)

    barrier = pltpu.get_barrier_semaphore()
    greeted = [up, down, z_peer(1), z_peer(-1)] + [p_peer(by) for by in range(1, PLANE)]
    for device in greeted:
        signal(barrier, device)

    def loads(layer):
        at = pl.ds(layer * rows, rows)
        pairs = [
            (pres_hbm.at[:, at], pres.at[:, at]),
            (adj_hbm.at[:, at], adj.at[:, at]),
            (perm_hbm.at[:, at], perm.at[:, at]),
            (act_hbm.at[at], act.at[at]),
            (code_hbm.at[:, at], code.at[:, at]),
        ]
        return [pltpu.make_async_copy(s, d, load_sem.at[i, layer]) for i, (s, d) in enumerate(pairs)]

    for layer in [0, layers - 1] + list(range(1, layers - 1)):
        for copy in loads(layer):
            copy.start()

    zero8 = jnp.zeros((8, rows), F32)
    for t in range(steps):
        pres[t, pl.ds(cells, 8), :] = zero8
        adj[t, pl.ds(cells, 8), :] = zero8
    for d in range(3):
        perm[d, pl.ds(cells, 8), :] = zero8
    act[pl.ds(cells, 8), :] = jnp.zeros((8, rows), jnp.int32)
    to_up_y[pl.ds(0, 8), :] = zero8

    def arrived(layer):
        for copy in loads(layer):
            copy.wait()

    arrived(0)
    arrived(layers - 1)

    low_a = pl.ds(0, half)
    top_b = pl.ds(top + half, half)

    def remote(src, dst, send, recv, device):
        return pltpu.make_async_remote_copy(
            src_ref=src, dst_ref=dst, send_sem=send, recv_sem=recv,
            device_id={"gx": device}, device_id_type=MESH,
        )

    goes_down = [
        remote(s, d, send_down.at[i], recv_down.at[i], down)
        for i, (s, d) in enumerate([
            (pres.at[:, low_a], above_pres),
            (adj.at[:, low_a], above_adj),
            (perm.at[0, low_a], above_perm),
            (act.at[low_a], above_act),
            (stage_low, above_log),
            (stage_rb, got_rb),
        ])
    ]
    goes_up = [
        remote(s, d, send_up.at[i], recv_up.at[i], up)
        for i, (s, d) in enumerate([
            (pres.at[:, top_b], below_pres),
            (adj.at[:, top_b], below_adj),
            (perm.at[0, top_b], below_perm),
            (stage_factor, below_factor),
            (stage_high, below_log),
            (stage_ra, got_ra),
        ])
    ]
    stage_factor[...] = multiplier(code[0, top_b, :]) * act[top_b, :].astype(F32)

    pl.semaphore_wait(barrier, len(greeted))
    for i in range(2):
        goes_up[i].start()
        goes_down[i].start()
    goes_up[2].start()
    goes_down[2].start()
    goes_down[3].start()

    def shake(round_, by):
        signal(hand.at[round_], z_peer(by))
        signal(hand.at[round_], z_peer(-by))

    shake(0, 1)

    lane = lax.broadcasted_iota(jnp.int32, (BLOCK, rows), 1)
    sub = lax.broadcasted_iota(jnp.int32, (BLOCK, rows), 0)
    z_open = jnp.where(lane == rows - 1, 0.0, 1.0).astype(F32)

    def fold(square):
        return jnp.sum(square.reshape(BLOCK // 8, 8, rows), axis=0)

    def block(start, in_layer, acc, from_below, to_above):
        at = pl.ds(start, BLOCK)
        next_row = pl.ds(start + 1, BLOCK)
        next_layer = pl.ds(start + rows, BLOCK)
        px = py = pz = None
        for t in range(steps):
            p, a = pres[t, at, :], adj[t, at, :]
            y = (a - adj[t, next_row, :]) * (p - pres[t, next_row, :])
            z = (a - pltpu.roll(a, rows - 1, 1)) * (p - pltpu.roll(p, rows - 1, 1))
            py = y if t == 0 else py + y
            pz = z if t == 0 else pz + z
            if to_above:
                x = (a - adj[t, next_layer, :]) * (p - pres[t, next_layer, :])
                px = x if t == 0 else px + x
        opened = act[at, :].astype(F32)

        k = perm[2, at, :]
        factor = multiplier(code[2, at, :]) * opened * pltpu.roll(opened, rows - 1, 1) * z_open
        mine, above = face(pz, factor, k, pltpu.roll(k, rows - 1, 1))
        log = k * (mine + pltpu.roll(above, 1, 1))
        log_ref[2, at, :] = log
        acc = acc + fold(log * log)

        k = perm[1, at, :]
        y_open = jnp.where(in_layer + sub == rows - 1, 0.0, 1.0).astype(F32)
        factor = multiplier(code[1, at, :]) * opened * act[next_row, :].astype(F32) * y_open
        mine, above = face(py, factor, k, perm[1, next_row, :])
        to_up_y[next_row, :] = above
        log = k * (mine + to_up_y[at, :])
        log_ref[1, at, :] = log
        acc = acc + fold(log * log)

        k = perm[0, at, :]
        total = None
        if to_above:
            factor = multiplier(code[0, at, :]) * opened * act[next_layer, :].astype(F32)
            mine, above = face(px, factor, k, perm[0, next_layer, :])
            to_up_x[next_layer, :] = above
            total = mine
        if from_below:
            into = to_up_x[at, :]
            total = into if total is None else total + into
        log = k * total
        log_ref[0, at, :] = log
        if from_below and to_above:
            acc = acc + fold(log * log)
        return acc

    def layer_of(layer, acc, from_below=True, to_above=True):
        def body(i, acc):
            in_layer = pl.multiple_of(i * BLOCK, BLOCK)
            return block(pl.multiple_of(layer * rows + in_layer, BLOCK), in_layer, acc, from_below, to_above)

        return lax.fori_loop(0, rows // BLOCK, body, acc)

    def middle(first, last, acc):
        def body(layer, acc):
            arrived(layer + 1)
            return layer_of(layer, acc)

        return lax.fori_loop(first, last, body, acc)

    arrived(1)
    acc = layer_of(0, jnp.zeros((8, rows), F32), from_below=False)
    stage_low[...] = log_ref[0, low_a, :]
    goes_up[3].start()
    pl.semaphore_wait(hand.at[0], 2)
    shake(1, 2)
    acc = middle(1, 3, acc)
    goes_down[4].start()
    pl.semaphore_wait(hand.at[1], 2)
    shake(2, 4)
    acc = middle(3, layers - 2, acc)
    acc = layer_of(layers - 2, acc)
    stage_high[...] = perm[0, top_b, :] * to_up_x[top_b, :]
    acc = layer_of(layers - 1, acc, to_above=False)
    goes_up[4].start()
    pl.semaphore_wait(hand.at[2], 2)

    not_last = jnp.where(me == n - 1, 0.0, 1.0).astype(F32)
    not_first = jnp.where(me == 0, 0.0, 1.0).astype(F32)

    def products_of(lower_pres, lower_adj, lower_at, upper_pres, upper_adj, upper_at):
        total = None
        for t in range(steps):
            term = (lower_adj[t, lower_at, :] - upper_adj[t, upper_at, :]) * (
                lower_pres[t, lower_at, :] - upper_pres[t, upper_at, :]
            )
            total = term if t == 0 else total + term
        return total

    for i in range(5):
        goes_down[i].wait_recv()
    for i in range(5):
        goes_up[i].wait_recv()

    def shared(i, acc):
        there = pl.ds(pl.multiple_of(i * BLOCK, BLOCK), BLOCK)
        here = pl.ds(pl.multiple_of(top + i * BLOCK, BLOCK), BLOCK)
        products = products_of(pres, adj, here, above_pres, above_adj, there)
        factor = multiplier(code[0, here, :]) * act[here, :].astype(F32) * above_act[there, :].astype(F32) * not_last
        k, k_up = perm[0, here, :], above_perm[there, :]
        mine, other = face(products, factor, k, k_up)
        log = log_ref[0, here, :] + k * mine
        log_ref[0, here, :] = log
        reply = k_up * other
        stage_ra[there, :] = reply
        reply = reply + above_log[there, :]
        acc = acc + fold(log * log) + fold(reply * reply)

        here = pl.ds(pl.multiple_of(half + i * BLOCK, BLOCK), BLOCK)
        products = products_of(below_pres, below_adj, there, pres, adj, here)
        factor = below_factor[there, :] * act[here, :].astype(F32) * not_first
        k, k_low = perm[0, here, :], below_perm[there, :]
        other, mine = face(products, factor, k_low, k)
        log = log_ref[0, here, :] + k * mine
        log_ref[0, here, :] = log
        reply = k_low * other
        stage_rb[there, :] = reply
        reply = reply + below_log[there, :]
        return acc + fold(log * log) + fold(reply * reply)

    acc = lax.fori_loop(0, half // BLOCK, shared, acc)

    def exchange(value, stage, buf, send, recv, mine, count, peer):
        stage[...] = value
        buf[mine] = value
        copies = []
        for by in range(1, count):
            copies.append(
                remote(stage, buf.at[mine], send.at[by], recv.at[by], peer(by))
            )
        order = sorted(range(1, count), key=lambda by: -min(by, count - by))
        for by in order:
            copies[by - 1].start()
        return copies

    copies_z = exchange(
        jnp.sum(acc, axis=0, keepdims=True), stage_z, buf_z, send_z, recv_z, my_z, planes, lambda by: z_peer(by)
    )
    goes_up[5].start()
    goes_down[5].start()
    for copy in copies_z:
        copy.wait_recv()
    copies_p = exchange(
        jnp.sum(buf_z[...], axis=0), stage_p, buf_p, send_p, recv_p, my_p, PLANE, p_peer
    )

    goes_down[5].wait_recv()
    goes_up[5].wait_recv()
    log_ref[0, low_a, :] += got_ra[...]
    log_ref[0, top_b, :] += got_rb[...]

    for copy in copies_p:
        copy.wait_recv()
    total = jnp.sum(jnp.sum(buf_p[...], axis=0), axis=1, keepdims=True)
    entries = 3 * cells * rows * n
    inv_ref[...] = jnp.broadcast_to(1.0 / jnp.sqrt(total / entries + epsilon), inv_ref.shape)

    for copy in copies_z + copies_p + goes_up + goes_down:
        copy.wait_send()


def local(n, pressure, adjoint, permeability, active, fault_codes):
    steps, layers, rows, lanes = pressure.shape
    cells = layers * rows
    half = rows // 2
    planes = n // PLANE
    vmem = pltpu.VMEM
    halo = [
        vmem((steps, half, lanes), F32),
        vmem((steps, half, lanes), F32),
        vmem((half, lanes), F32),
    ]
    tile = vmem((half, lanes), F32)
    scratch = [
        vmem((steps, cells + 8, lanes), F32),
        vmem((steps, cells + 8, lanes), F32),
        vmem((3, cells + 8, lanes), F32),
        vmem((cells + 8, lanes), jnp.int32),
        vmem((3, cells, lanes), jnp.int32),
        vmem((cells, lanes), F32),
        vmem((cells + 8, lanes), F32),
        *halo, vmem((half, lanes), jnp.int32), tile,
        *halo, tile, tile,
        tile, tile, tile, tile, tile, tile, tile,
        vmem((1, lanes), F32), vmem((planes, 1, lanes), F32),
        vmem((1, lanes), F32), vmem((PLANE, 1, lanes), F32),
        pltpu.SemaphoreType.DMA((5, layers)),
        pltpu.SemaphoreType.DMA((6,)), pltpu.SemaphoreType.DMA((6,)),
        pltpu.SemaphoreType.DMA((6,)), pltpu.SemaphoreType.DMA((6,)),
        pltpu.SemaphoreType.DMA((planes,)), pltpu.SemaphoreType.DMA((planes,)),
        pltpu.SemaphoreType.DMA((PLANE,)), pltpu.SemaphoreType.DMA((PLANE,)),
        pltpu.SemaphoreType.REGULAR((3,)),
    ]
    hbm = pl.BlockSpec(memory_space=pltpu.HBM)
    in_hbm = lambda x: pltpu.with_memory_space_constraint(x, pltpu.HBM)
    log, inverse = pl.pallas_call(
        functools.partial(kernel, steps, layers, rows, n),
        out_shape=(
            jax.ShapeDtypeStruct((3, cells, lanes), F32),
            jax.ShapeDtypeStruct((1, lanes), F32),
        ),
        in_specs=[hbm] * 5,
        out_specs=(pl.BlockSpec(memory_space=pltpu.VMEM), pl.BlockSpec(memory_space=pltpu.VMEM)),
        scratch_shapes=scratch,
        compiler_params=pltpu.CompilerParams(
            collective_id=0, has_side_effects=True, vmem_limit_bytes=32 * 1024 * 1024
        ),
        name="gradient",
    )(
        in_hbm(pressure.reshape(steps, cells, lanes)),
        in_hbm(adjoint.reshape(steps, cells, lanes)),
        in_hbm(permeability.reshape(3, cells, lanes)),
        in_hbm(active.reshape(cells, lanes)),
        in_hbm(fault_codes.reshape(3, cells, lanes)),
    )
    out = log * inverse[None]
    return out.reshape(3, layers, rows, lanes)


def solution(mesh):
    n = mesh.shape["gx"]
    whole = ("groups", "gx")
    four = P(None, whole, None, None)
    return jax.shard_map(
        functools.partial(local, n),
        mesh=mesh,
        in_specs=(four, four, four, P(whole, None, None), four),
        out_specs=four,
        check_vma=False,
    )
```

```python
import functools

import jax
import jax.numpy as jnp
from jax import lax
from jax.experimental import pallas as pl
from jax.experimental.pallas import tpu as pltpu
from jax.sharding import PartitionSpec as P

MESH = pl.DeviceIdType.MESH
F32 = jnp.float32

epsilon = 1e-06

PLANE = 8
BLOCK = 32


def multiplier(codes):
    return jnp.where(codes == 0, 1.0, jnp.where(codes == 1, 0.6, jnp.where(codes == 2, 0.25, 0.05)))


def face(products, factor, lower_perm, upper_perm):
    inverse = 1.0 / (lower_perm + upper_perm)
    weight = (2.0 * factor) * products
    upper = upper_perm * inverse
    lower = lower_perm * inverse
    return weight * upper * upper, weight * lower * lower


def kernel(
    steps, layers, rows, n,
    pres_hbm, adj_hbm, perm_hbm, act_hbm, code_hbm,
    log_ref, inv_ref,
    pres, adj, perm, act, code,
    to_up_x, to_up_y,
    above_pres, above_adj, above_perm, above_act, above_log,
    below_pres, below_adj, below_perm, below_factor, below_log,
    stage_factor, stage_low, stage_high, stage_ra, stage_rb, got_ra, got_rb,
    stage_sum, sums, stage_inv, got_inv,
    load_sem, send_up, recv_up, send_down, recv_down,
    send_sum, recv_sum, send_inv, recv_inv,
):
    half = rows // 2
    cells = layers * rows
    top = cells - rows
    planes = n // PLANE
    me = lax.axis_index("gx")
    root = me < PLANE
    first, last = me == 0, me == n - 1
    up = lax.rem(me + 1, n)
    down = lax.rem(me + n - 1, n)

    barrier = pltpu.get_barrier_semaphore()

    def greet(device):
        pl.semaphore_signal(barrier, inc=1, device_id={"gx": device}, device_id_type=MESH)

    @pl.when(jnp.logical_not(last))
    def _():
        greet(up)

    @pl.when(jnp.logical_not(first))
    def _():
        greet(down)

    groups = [(0, 1), (layers - 1, 1), (1, 1), (2, 2), (4, layers - 5)]

    def loads(group):
        layer, count = groups[group]
        at = pl.ds(layer * rows, count * rows)
        pairs = [
            (pres_hbm.at[:, at], pres.at[:, at]),
            (adj_hbm.at[:, at], adj.at[:, at]),
            (perm_hbm.at[:, at], perm.at[:, at]),
            (act_hbm.at[at], act.at[at]),
            (code_hbm.at[:, at], code.at[:, at]),
        ]
        return [pltpu.make_async_copy(s, d, load_sem.at[group, i]) for i, (s, d) in enumerate(pairs)]

    loaded = [loads(group) for group in range(len(groups))]
    for copies in loaded:
        for copy in copies:
            copy.start()

    def arrived(group):
        for copy in loaded[group]:
            copy.wait()

    @pl.when(root)
    def _():
        def body(i, carry):
            greet(lax.rem(me + i, n))
            return carry

        lax.fori_loop(1, n, body, 0)

    zero8 = jnp.zeros((8, rows), F32)
    for t in range(steps):
        pres[t, pl.ds(cells, 8), :] = zero8
        adj[t, pl.ds(cells, 8), :] = zero8
    for d in range(3):
        perm[d, pl.ds(cells, 8), :] = zero8
    act[pl.ds(cells, 8), :] = jnp.zeros((8, rows), jnp.int32)
    to_up_y[pl.ds(0, 8), :] = zero8

    arrived(0)
    arrived(1)

    low_a = pl.ds(0, half)
    top_b = pl.ds(top + half, half)

    def remote(src, dst, send, recv, device):
        return pltpu.make_async_remote_copy(
            src_ref=src, dst_ref=dst, send_sem=send, recv_sem=recv,
            device_id={"gx": device}, device_id_type=MESH,
        )

    goes_down = [
        remote(s, d, send_down.at[i], recv_down.at[i], down)
        for i, (s, d) in enumerate([
            (pres.at[:, low_a], above_pres),
            (adj.at[:, low_a], above_adj),
            (perm.at[0, low_a], above_perm),
            (act.at[low_a], above_act),
            (stage_low, above_log),
            (stage_rb, got_rb),
        ])
    ]
    goes_up = [
        remote(s, d, send_up.at[i], recv_up.at[i], up)
        for i, (s, d) in enumerate([
            (pres.at[:, top_b], below_pres),
            (adj.at[:, top_b], below_adj),
            (perm.at[0, top_b], below_perm),
            (stage_factor, below_factor),
            (stage_high, below_log),
            (stage_ra, got_ra),
        ])
    ]
    stage_factor[...] = multiplier(code[0, top_b, :]) * act[top_b, :].astype(F32)

    def one_if(condition):
        return jnp.where(condition, 1, 0)

    pl.semaphore_wait(barrier, 2 + PLANE - one_if(first) - one_if(last) - one_if(root))

    def start(parts):
        @pl.when(jnp.logical_not(last))
        def _():
            for i in parts:
                goes_up[i].start()

        @pl.when(jnp.logical_not(first))
        def _():
            for i in parts:
                goes_down[i].start()

    start([0, 1, 2, 3])

    lane = lax.broadcasted_iota(jnp.int32, (BLOCK, rows), 1)
    sub = lax.broadcasted_iota(jnp.int32, (BLOCK, rows), 0)
    z_open = jnp.where(lane == rows - 1, 0.0, 1.0).astype(F32)

    def fold(square):
        return jnp.sum(square.reshape(BLOCK // 8, 8, rows), axis=0)

    def block(start, in_layer, acc, from_below, to_above):
        at = pl.ds(start, BLOCK)
        next_row = pl.ds(start + 1, BLOCK)
        next_layer = pl.ds(start + rows, BLOCK)
        px = py = pz = None
        for t in range(steps):
            p, a = pres[t, at, :], adj[t, at, :]
            y = (a - adj[t, next_row, :]) * (p - pres[t, next_row, :])
            z = (a - pltpu.roll(a, rows - 1, 1)) * (p - pltpu.roll(p, rows - 1, 1))
            py = y if t == 0 else py + y
            pz = z if t == 0 else pz + z
            if to_above:
                x = (a - adj[t, next_layer, :]) * (p - pres[t, next_layer, :])
                px = x if t == 0 else px + x
        opened = act[at, :].astype(F32)

        k = perm[2, at, :]
        factor = multiplier(code[2, at, :]) * opened * pltpu.roll(opened, rows - 1, 1) * z_open
        mine, above = face(pz, factor, k, pltpu.roll(k, rows - 1, 1))
        log = k * (mine + pltpu.roll(above, 1, 1))
        log_ref[2, at, :] = log
        acc = acc + fold(log * log)

        k = perm[1, at, :]
        y_open = jnp.where(in_layer + sub == rows - 1, 0.0, 1.0).astype(F32)
        factor = multiplier(code[1, at, :]) * opened * act[next_row, :].astype(F32) * y_open
        mine, above = face(py, factor, k, perm[1, next_row, :])
        to_up_y[next_row, :] = above
        log = k * (mine + to_up_y[at, :])
        log_ref[1, at, :] = log
        acc = acc + fold(log * log)

        k = perm[0, at, :]
        total = None
        if to_above:
            factor = multiplier(code[0, at, :]) * opened * act[next_layer, :].astype(F32)
            mine, above = face(px, factor, k, perm[0, next_layer, :])
            to_up_x[next_layer, :] = above
            total = mine
        if from_below:
            into = to_up_x[at, :]
            total = into if total is None else total + into
        log = k * total
        log_ref[0, at, :] = log
        if from_below and to_above:
            acc = acc + fold(log * log)
        return acc

    def layer_of(layer, acc, from_below=True, to_above=True):
        def body(i, acc):
            in_layer = pl.multiple_of(i * BLOCK, BLOCK)
            return block(pl.multiple_of(layer * rows + in_layer, BLOCK), in_layer, acc, from_below, to_above)

        return lax.fori_loop(0, rows // BLOCK, body, acc)

    def middle(begin, end, acc):
        return lax.fori_loop(begin, end, layer_of, acc)

    arrived(2)
    acc = layer_of(0, jnp.zeros((8, rows), F32), from_below=False)
    stage_low[...] = log_ref[0, low_a, :]
    arrived(3)
    acc = middle(1, 3, acc)
    arrived(4)
    acc = middle(3, layers - 1, acc)
    stage_high[...] = perm[0, top_b, :] * to_up_x[top_b, :]
    acc = layer_of(layers - 1, acc, to_above=False)
    start([4])

    def products_of(lower_pres, lower_adj, lower_at, upper_pres, upper_adj, upper_at):
        total = None
        for t in range(steps):
            term = (lower_adj[t, lower_at, :] - upper_adj[t, upper_at, :]) * (
                lower_pres[t, lower_at, :] - upper_pres[t, upper_at, :]
            )
            total = term if t == 0 else total + term
        return total

    def received(parts):
        @pl.when(jnp.logical_not(last))
        def _():
            for i in parts:
                goes_down[i].wait_recv()

        @pl.when(jnp.logical_not(first))
        def _():
            for i in parts:
                goes_up[i].wait_recv()

    received(range(5))

    def keep(condition, value):
        return jnp.where(condition, value, 0.0)

    def shared(i, acc):
        there = pl.ds(pl.multiple_of(i * BLOCK, BLOCK), BLOCK)
        here = pl.ds(pl.multiple_of(top + i * BLOCK, BLOCK), BLOCK)
        inside = jnp.logical_not(last)
        products = products_of(pres, adj, here, above_pres, above_adj, there)
        factor = multiplier(code[0, here, :]) * act[here, :].astype(F32) * above_act[there, :].astype(F32)
        k, k_up = perm[0, here, :], above_perm[there, :]
        mine, other = face(products, factor, k, k_up)
        log = log_ref[0, here, :] + keep(inside, k * mine)
        log_ref[0, here, :] = log
        reply = k_up * other
        stage_ra[there, :] = reply
        reply = keep(inside, reply + above_log[there, :])
        end = keep(last, log_ref[0, pl.ds(pl.multiple_of(top + half + i * BLOCK, BLOCK), BLOCK), :])
        acc = acc + fold(log * log) + fold(reply * reply) + fold(end * end)

        here = pl.ds(pl.multiple_of(half + i * BLOCK, BLOCK), BLOCK)
        inside = jnp.logical_not(first)
        products = products_of(below_pres, below_adj, there, pres, adj, here)
        factor = below_factor[there, :] * act[here, :].astype(F32)
        k, k_low = perm[0, here, :], below_perm[there, :]
        other, mine = face(products, factor, k_low, k)
        log = log_ref[0, here, :] + keep(inside, k * mine)
        log_ref[0, here, :] = log
        reply = k_low * other
        stage_rb[there, :] = reply
        reply = keep(inside, reply + below_log[there, :])
        end = keep(first, log_ref[0, there, :])
        return acc + fold(log * log) + fold(reply * reply) + fold(end * end)

    acc = lax.fori_loop(0, half // BLOCK, shared, acc)

    partial = jnp.sum(acc, axis=0, keepdims=True)
    stage_sum[...] = partial
    to_roots = [
        remote(stage_sum, sums.at[me], send_sum.at[q], recv_sum, q) for q in range(PLANE)
    ]
    for q in range(PLANE):
        @pl.when(me != q)
        def _():
            to_roots[q].start()

    start([5])
    received([5])

    @pl.when(jnp.logical_not(first))
    def _():
        log_ref[0, low_a, :] += got_ra[...]

    @pl.when(jnp.logical_not(last))
    def _():
        log_ref[0, top_b, :] += got_rb[...]

    @pl.when(root)
    def _():
        sums[me] = partial
        others = sums.at[pl.ds(0, n - 1)]
        pltpu.make_async_copy(others, others, recv_sum).wait()
        quarter = n // 4
        total = sum(jnp.sum(sums[pl.ds(q * quarter, quarter)], axis=0) for q in range(4))
        total = jnp.sum(total, axis=1, keepdims=True)
        entries = 3 * cells * rows * n
        inverse = jnp.broadcast_to(1.0 / jnp.sqrt(total / entries + epsilon), inv_ref.shape)
        stage_inv[...] = inverse
        copies = [
            remote(stage_inv, got_inv, send_inv.at[z], recv_inv, me + z * PLANE) for z in range(1, planes)
        ]
        for copy in copies:
            copy.start()
        inv_ref[...] = inverse
        for copy in copies:
            copy.wait_send()

    @pl.when(jnp.logical_not(root))
    def _():
        remote(stage_inv, got_inv, send_inv.at[0], recv_inv, me).wait_recv()
        inv_ref[...] = got_inv[...]

    for q in range(PLANE):
        @pl.when(me != q)
        def _():
            to_roots[q].wait_send()

    @pl.when(jnp.logical_not(last))
    def _():
        for copy in goes_up:
            copy.wait_send()

    @pl.when(jnp.logical_not(first))
    def _():
        for copy in goes_down:
            copy.wait_send()


def local(n, pressure, adjoint, permeability, active, fault_codes):
    steps, layers, rows, lanes = pressure.shape
    cells = layers * rows
    half = rows // 2
    planes = n // PLANE
    vmem = pltpu.VMEM
    halo = [
        vmem((steps, half, lanes), F32),
        vmem((steps, half, lanes), F32),
        vmem((half, lanes), F32),
    ]
    tile = vmem((half, lanes), F32)
    scratch = [
        vmem((steps, cells + 8, lanes), F32),
        vmem((steps, cells + 8, lanes), F32),
        vmem((3, cells + 8, lanes), F32),
        vmem((cells + 8, lanes), jnp.int32),
        vmem((3, cells, lanes), jnp.int32),
        vmem((cells, lanes), F32),
        vmem((cells + 8, lanes), F32),
        *halo, vmem((half, lanes), jnp.int32), tile,
        *halo, tile, tile,
        tile, tile, tile, tile, tile, tile, tile,
        vmem((1, lanes), F32), vmem((n, 1, lanes), F32),
        vmem((1, lanes), F32), vmem((1, lanes), F32),
        pltpu.SemaphoreType.DMA((5, 5)),
        pltpu.SemaphoreType.DMA((6,)), pltpu.SemaphoreType.DMA((6,)),
        pltpu.SemaphoreType.DMA((6,)), pltpu.SemaphoreType.DMA((6,)),
        pltpu.SemaphoreType.DMA((PLANE,)), pltpu.SemaphoreType.DMA,
        pltpu.SemaphoreType.DMA((planes,)), pltpu.SemaphoreType.DMA,
    ]
    hbm = pl.BlockSpec(memory_space=pltpu.HBM)
    in_hbm = lambda x: pltpu.with_memory_space_constraint(x, pltpu.HBM)
    log, inverse = pl.pallas_call(
        functools.partial(kernel, steps, layers, rows, n),
        out_shape=(
            jax.ShapeDtypeStruct((3, cells, lanes), F32),
            jax.ShapeDtypeStruct((1, lanes), F32),
        ),
        in_specs=[hbm] * 5,
        out_specs=(pl.BlockSpec(memory_space=pltpu.VMEM), pl.BlockSpec(memory_space=pltpu.VMEM)),
        scratch_shapes=scratch,
        compiler_params=pltpu.CompilerParams(
            collective_id=0, has_side_effects=True, vmem_limit_bytes=32 * 1024 * 1024
        ),
        name="gradient",
    )(
        in_hbm(pressure.reshape(steps, cells, lanes)),
        in_hbm(adjoint.reshape(steps, cells, lanes)),
        in_hbm(permeability.reshape(3, cells, lanes)),
        in_hbm(active.reshape(cells, lanes)),
        in_hbm(fault_codes.reshape(3, cells, lanes)),
    )
    out = log * inverse[None]
    return out.reshape(3, layers, rows, lanes)


def solution(mesh):
    n = mesh.shape["gx"]
    whole = ("groups", "gx")
    four = P(None, whole, None, None)
    return jax.shard_map(
        functools.partial(local, n),
        mesh=mesh,
        in_specs=(four, four, four, P(whole, None, None), four),
        out_specs=four,
        check_vma=False,
    )
```

```python
import functools

import jax
import jax.numpy as jnp
from jax import lax
from jax.experimental import pallas as pl
from jax.experimental.pallas import tpu as pltpu
from jax.sharding import PartitionSpec as P

MESH = pl.DeviceIdType.MESH
F32 = jnp.float32

epsilon = 1e-06

PLANE = 8
BLOCK = 32


def multiplier(codes):
    return jnp.where(codes == 0, 1.0, jnp.where(codes == 1, 0.6, jnp.where(codes == 2, 0.25, 0.05)))


def face(products, factor, lower_perm, upper_perm):
    inverse = 1.0 / (lower_perm + upper_perm)
    weight = (2.0 * factor) * products
    upper = upper_perm * inverse
    lower = lower_perm * inverse
    return weight * upper * upper, weight * lower * lower


def kernel(
    steps, layers, rows, n,
    pres_hbm, adj_hbm, perm_hbm, act_hbm, code_hbm,
    log_ref, inv_ref,
    pres, adj, perm, act, code,
    to_up_x, to_up_y,
    above_pres, above_adj, above_perm, above_log,
    below_pres, below_adj, below_perm, below_factor, below_log,
    stage_factor, stage_perm, stage_low, stage_high, stage_ra, stage_rb, got_ra, got_rb,
    stage_sum, sums, stage_inv, got_inv,
    load_sem, send_up, recv_up, send_down, recv_down,
    send_sum, recv_sum, send_inv, send_extra, recv_inv,
):
    half = rows // 2
    cells = layers * rows
    top = cells - rows
    planes = n // PLANE
    takers = 2 * PLANE - 1
    me = lax.axis_index("gx")
    first, last = me == 0, me == n - 1
    taker = jnp.logical_and(me >= 1, me <= takers)
    up, down = me + 1, me - 1

    def wait_rows(sem, row_count, wide=1):
        ref = pres.at[pl.ds(0, wide), pl.ds(0, row_count // wide)]
        pltpu.make_async_copy(ref, ref, sem).wait()

    def load(group, parts):
        for src, dst, begin, count in parts:
            at = pl.ds(begin, count)
            where = (at,) if len(src.shape) == 2 else (slice(None), at)
            pltpu.make_async_copy(src.at[where], dst.at[where], load_sem.at[group]).start()

    fields = [(pres_hbm, pres), (adj_hbm, adj)]
    others = [(perm_hbm, perm), (act_hbm, act), (code_hbm, code)]

    def span(refs, begin, end):
        return [(src, dst, begin, end - begin) for src, dst in refs]

    load(0, span(fields, 0, half) + span(fields, top + half, cells))

    barrier = pltpu.get_barrier_semaphore()

    def greet(device):
        pl.semaphore_signal(barrier, inc=1, device_id={"gx": device}, device_id_type=MESH)

    @pl.when(jnp.logical_not(last))
    def _():
        greet(up)

    @pl.when(jnp.logical_not(first))
    def _():
        greet(down)

    @pl.when(taker)
    def _():
        def body(device, carry):
            @pl.when(device != me)
            def _():
                greet(device)

            return carry

        lax.fori_loop(0, n, body, 0)

    zero8 = jnp.zeros((8, rows), F32)
    for t in range(steps):
        pres[t, pl.ds(cells, 8), :] = zero8
        adj[t, pl.ds(cells, 8), :] = zero8
    for d in range(3):
        perm[d, pl.ds(cells, 8), :] = zero8
    act[pl.ds(cells, 8), :] = jnp.zeros((8, rows), jnp.int32)
    to_up_y[pl.ds(0, 8), :] = zero8

    low_a = pl.ds(0, half)
    top_b = pl.ds(top + half, half)

    def remote(src, dst, send, recv, device):
        return pltpu.make_async_remote_copy(
            src_ref=src, dst_ref=dst, send_sem=send, recv_sem=recv,
            device_id={"gx": device}, device_id_type=MESH,
        )

    goes_down = [
        remote(s, d, send_down, recv_down.at[int(i == 4)], down)
        for i, (s, d) in enumerate([
            (pres.at[:, low_a], above_pres),
            (adj.at[:, low_a], above_adj),
            (stage_perm, above_perm),
            (stage_low, above_log),
            (stage_rb, got_rb),
        ])
    ]
    goes_up = [
        remote(s, d, send_up, recv_up.at[int(i == 5)], up)
        for i, (s, d) in enumerate([
            (pres.at[:, top_b], below_pres),
            (adj.at[:, top_b], below_adj),
            (perm.at[0, top_b], below_perm),
            (stage_factor, below_factor),
            (stage_high, below_log),
            (stage_ra, got_ra),
        ])
    ]

    def start_up(*parts):
        @pl.when(jnp.logical_not(last))
        def _():
            for i in parts:
                goes_up[i].start()

    def start_down(*parts):
        @pl.when(jnp.logical_not(first))
        def _():
            for i in parts:
                goes_down[i].start()

    def one_if(condition):
        return jnp.where(condition, 1, 0)

    wait_rows(load_sem.at[0], 4 * steps * half, steps)
    pl.semaphore_wait(barrier, 2 + takers - one_if(first) - one_if(last) - one_if(taker))
    start_up(0, 1)
    start_down(0, 1)

    load(1, span(fields, half, 2 * rows) + span(others, 0, 2 * rows))
    load(2, span(fields + others, 2 * rows, 4 * rows))
    load(3, span(fields + others, 4 * rows, 6 * rows))
    load(4, span(fields, 6 * rows, top + half) + span(others, 6 * rows, cells))
    edge = 2 * steps * (2 * rows - half) + 7 * 2 * rows
    whole = (2 * steps + 7) * 2 * rows

    lane = lax.broadcasted_iota(jnp.int32, (BLOCK, rows), 1)
    sub = lax.broadcasted_iota(jnp.int32, (BLOCK, rows), 0)
    z_open = jnp.where(lane == rows - 1, 0.0, 1.0).astype(F32)

    def fold(square):
        return jnp.sum(square.reshape(BLOCK // 8, 8, rows), axis=0)

    def block(start, in_layer, acc, from_below, to_above):
        at = pl.ds(start, BLOCK)
        next_row = pl.ds(start + 1, BLOCK)
        next_layer = pl.ds(start + rows, BLOCK)
        px = py = pz = None
        for t in range(steps):
            p, a = pres[t, at, :], adj[t, at, :]
            y = (a - adj[t, next_row, :]) * (p - pres[t, next_row, :])
            z = (a - pltpu.roll(a, rows - 1, 1)) * (p - pltpu.roll(p, rows - 1, 1))
            py = y if t == 0 else py + y
            pz = z if t == 0 else pz + z
            if to_above:
                x = (a - adj[t, next_layer, :]) * (p - pres[t, next_layer, :])
                px = x if t == 0 else px + x
        opened = act[at, :].astype(F32)

        k = perm[2, at, :]
        factor = multiplier(code[2, at, :]) * opened * pltpu.roll(opened, rows - 1, 1) * z_open
        mine, above = face(pz, factor, k, pltpu.roll(k, rows - 1, 1))
        log = k * (mine + pltpu.roll(above, 1, 1))
        log_ref[2, at, :] = log
        acc = acc + fold(log * log)

        k = perm[1, at, :]
        y_open = jnp.where(in_layer + sub == rows - 1, 0.0, 1.0).astype(F32)
        factor = multiplier(code[1, at, :]) * opened * act[next_row, :].astype(F32) * y_open
        mine, above = face(py, factor, k, perm[1, next_row, :])
        to_up_y[next_row, :] = above
        log = k * (mine + to_up_y[at, :])
        log_ref[1, at, :] = log
        acc = acc + fold(log * log)

        k = perm[0, at, :]
        total = None
        if to_above:
            factor = multiplier(code[0, at, :]) * opened * act[next_layer, :].astype(F32)
            mine, above = face(px, factor, k, perm[0, next_layer, :])
            to_up_x[next_layer, :] = above
            total = mine
        if from_below:
            into = to_up_x[at, :]
            total = into if total is None else total + into
        log = k * total
        log_ref[0, at, :] = log
        if from_below and to_above:
            acc = acc + fold(log * log)
        return acc

    def layer_of(layer, acc, from_below=True, to_above=True):
        def body(i, acc):
            in_layer = pl.multiple_of(i * BLOCK, BLOCK)
            return block(pl.multiple_of(layer * rows + in_layer, BLOCK), in_layer, acc, from_below, to_above)

        return lax.fori_loop(0, rows // BLOCK, body, acc)

    def middle(begin, end, acc):
        return lax.fori_loop(begin, end, layer_of, acc)

    wait_rows(load_sem.at[1], edge, steps)
    stage_perm[...] = perm[0, low_a, :] * act[low_a, :].astype(F32)
    acc = layer_of(0, jnp.zeros((8, rows), F32), from_below=False)
    start_down(2)
    stage_low[...] = log_ref[0, low_a, :]
    wait_rows(load_sem.at[2], whole, steps)
    acc = middle(1, 3, acc)
    start_down(3)
    wait_rows(load_sem.at[3], whole, steps)
    acc = middle(3, 5, acc)
    wait_rows(load_sem.at[4], edge, steps)
    start_up(2)
    stage_factor[...] = multiplier(code[0, top_b, :]) * act[top_b, :].astype(F32)
    acc = middle(5, layers - 1, acc)
    start_up(3)
    stage_high[...] = perm[0, top_b, :] * to_up_x[top_b, :]
    acc = layer_of(layers - 1, acc, to_above=False)
    start_up(4)

    def products_of(lower_pres, lower_adj, lower_at, upper_pres, upper_adj, upper_at):
        total = None
        for t in range(steps):
            term = (lower_adj[t, lower_at, :] - upper_adj[t, upper_at, :]) * (
                lower_pres[t, lower_at, :] - upper_pres[t, upper_at, :]
            )
            total = term if t == 0 else total + term
        return total

    @pl.when(jnp.logical_not(last))
    def _():
        wait_rows(recv_down.at[0], (2 * steps + 2) * half, 2)

    @pl.when(jnp.logical_not(first))
    def _():
        wait_rows(recv_up.at[0], (2 * steps + 3) * half, 2)

    def keep(condition, value):
        return jnp.where(condition, value, 0.0)

    def shared(i, acc):
        there = pl.ds(pl.multiple_of(i * BLOCK, BLOCK), BLOCK)
        here = pl.ds(pl.multiple_of(top + i * BLOCK, BLOCK), BLOCK)
        inside = jnp.logical_not(last)
        products = products_of(pres, adj, here, above_pres, above_adj, there)
        factor = multiplier(code[0, here, :]) * act[here, :].astype(F32)
        k, k_up = perm[0, here, :], above_perm[there, :]
        mine, other = face(products, factor, k, k_up)
        log = log_ref[0, here, :] + keep(inside, k * mine)
        log_ref[0, here, :] = log
        reply = k_up * other
        stage_ra[there, :] = reply
        reply = keep(inside, reply + above_log[there, :])
        end = keep(last, log_ref[0, pl.ds(pl.multiple_of(top + half + i * BLOCK, BLOCK), BLOCK), :])
        acc = acc + fold(log * log) + fold(reply * reply) + fold(end * end)

        here = pl.ds(pl.multiple_of(half + i * BLOCK, BLOCK), BLOCK)
        inside = jnp.logical_not(first)
        products = products_of(below_pres, below_adj, there, pres, adj, here)
        factor = below_factor[there, :] * act[here, :].astype(F32)
        k, k_low = perm[0, here, :], below_perm[there, :]
        other, mine = face(products, factor, k_low, k)
        log = log_ref[0, here, :] + keep(inside, k * mine)
        log_ref[0, here, :] = log
        reply = k_low * other
        stage_rb[there, :] = reply
        reply = keep(inside, reply + below_log[there, :])
        end = keep(first, log_ref[0, there, :])
        return acc + fold(log * log) + fold(reply * reply) + fold(end * end)

    acc = lax.fori_loop(0, half // BLOCK, shared, acc)

    partial = jnp.sum(acc, axis=0, keepdims=True)
    stage_sum[...] = partial
    to_takers = [remote(stage_sum, sums.at[me], send_sum, recv_sum, q) for q in range(1, takers + 1)]

    @pl.when(jnp.logical_not(taker))
    def _():
        for copy in to_takers:
            copy.start()

    @pl.when(taker)
    def _():
        for q in range(1, takers + 1):
            @pl.when(me != q)
            def _():
                to_takers[q - 1].start()

    start_up(5)
    start_down(4)

    @pl.when(jnp.logical_not(first))
    def _():
        wait_rows(recv_up.at[1], half)
        log_ref[0, low_a, :] += got_ra[...]
        wait_rows(send_down, (2 * steps + 3) * half, 2)

    @pl.when(jnp.logical_not(last))
    def _():
        wait_rows(recv_down.at[1], half)
        log_ref[0, top_b, :] += got_rb[...]
        wait_rows(send_up, (2 * steps + 4) * half, 2)

    @pl.when(taker)
    def _():
        wait_rows(send_sum, takers - 1)
        sums[me] = partial
        wait_rows(recv_sum, n - 1)
        quarter = n // 4
        total = sum(jnp.sum(sums[pl.ds(q * quarter, quarter)], axis=0) for q in range(4))
        total = jnp.sum(total, axis=1, keepdims=True)
        entries = 3 * cells * rows * n
        inverse = jnp.broadcast_to(1.0 / jnp.sqrt(total / entries + epsilon), inv_ref.shape)
        inv_ref[...] = inverse

        @pl.when(me >= PLANE)
        def _():
            stage_inv[...] = inverse
            for z in range(1, planes - 1):
                remote(stage_inv, got_inv, send_inv, recv_inv, me + z * PLANE).start()
            to_first = remote(stage_inv, got_inv, send_extra, recv_inv, 0)

            @pl.when(me == PLANE)
            def _():
                to_first.start()
                to_first.wait_send()

            wait_rows(send_inv, planes - 2)

    @pl.when(jnp.logical_not(taker))
    def _():
        wait_rows(send_sum, takers)
        wait_rows(recv_inv, 1)
        inv_ref[...] = got_inv[...]


def local(n, pressure, adjoint, permeability, active, fault_codes):
    steps, layers, rows, lanes = pressure.shape
    cells = layers * rows
    half = rows // 2
    planes = n // PLANE
    vmem, dma = pltpu.VMEM, pltpu.SemaphoreType.DMA
    halo = [
        vmem((steps, half, lanes), F32),
        vmem((steps, half, lanes), F32),
        vmem((half, lanes), F32),
    ]
    tile = vmem((half, lanes), F32)
    scratch = [
        vmem((steps, cells + 8, lanes), F32),
        vmem((steps, cells + 8, lanes), F32),
        vmem((3, cells + 8, lanes), F32),
        vmem((cells + 8, lanes), jnp.int32),
        vmem((3, cells, lanes), jnp.int32),
        vmem((cells, lanes), F32),
        vmem((cells + 8, lanes), F32),
        *halo, tile,
        *halo, tile, tile,
        tile, tile, tile, tile, tile, tile, tile, tile,
        vmem((1, lanes), F32), vmem((n, 1, lanes), F32),
        vmem((1, lanes), F32), vmem((1, lanes), F32),
        dma((5,)), dma, dma((2,)), dma, dma((2,)),
        dma, dma, dma, dma, dma,
    ]
    hbm = pl.BlockSpec(memory_space=pltpu.HBM)
    in_hbm = lambda x: pltpu.with_memory_space_constraint(x, pltpu.HBM)
    log, inverse = pl.pallas_call(
        functools.partial(kernel, steps, layers, rows, n),
        out_shape=(
            jax.ShapeDtypeStruct((3, cells, lanes), F32),
            jax.ShapeDtypeStruct((1, lanes), F32),
        ),
        in_specs=[hbm] * 5,
        out_specs=(pl.BlockSpec(memory_space=pltpu.VMEM), pl.BlockSpec(memory_space=pltpu.VMEM)),
        scratch_shapes=scratch,
        compiler_params=pltpu.CompilerParams(
            collective_id=0, has_side_effects=True, vmem_limit_bytes=32 * 1024 * 1024
        ),
        name="gradient",
    )(
        in_hbm(pressure.reshape(steps, cells, lanes)),
        in_hbm(adjoint.reshape(steps, cells, lanes)),
        in_hbm(permeability.reshape(3, cells, lanes)),
        in_hbm(active.reshape(cells, lanes)),
        in_hbm(fault_codes.reshape(3, cells, lanes)),
    )
    out = log * inverse[None]
    return out.reshape(3, layers, rows, lanes)


def solution(mesh):
    n = mesh.shape["gx"]
    whole = ("groups", "gx")
    four = P(None, whole, None, None)
    return jax.shard_map(
        functools.partial(local, n),
        mesh=mesh,
        in_specs=(four, four, four, P(whole, None, None), four),
        out_specs=four,
        check_vma=False,
    )
```

```python
import functools

import jax
import jax.numpy as jnp
from jax import lax
from jax.experimental import pallas as pl
from jax.experimental.pallas import tpu as pltpu
from jax.sharding import PartitionSpec as P

MESH = pl.DeviceIdType.MESH
F32 = jnp.float32

epsilon = 1e-06

PLANE = 8
BLOCK = 64
SHARED = 32


def multiplier(codes):
    return jnp.where(codes == 0, 1.0, jnp.where(codes == 1, 0.6, jnp.where(codes == 2, 0.25, 0.05)))


def face(products, factor, lower_perm, upper_perm):
    inverse = 1.0 / (lower_perm + upper_perm)
    weight = (2.0 * factor) * products
    upper = upper_perm * inverse
    lower = lower_perm * inverse
    return weight * upper * upper, weight * lower * lower


def kernel(
    steps, layers, rows, n,
    pres_hbm, adj_hbm, perm_hbm, act_hbm, code_hbm,
    log_ref, inv_ref,
    pres, adj, perm, act, code,
    to_up_x, to_up_y,
    above_pres, above_adj, above_perm, above_log,
    below_pres, below_adj, below_perm, below_factor, below_log,
    stage_factor, stage_perm, stage_low, stage_high, stage_ra, stage_rb, got_ra, got_rb,
    stage_sum, sums, stage_inv, got_inv,
    load_sem, send_up, recv_up, send_down, recv_down,
    send_sum, recv_sum, send_inv, send_first, recv_inv,
):
    half = rows // 2
    cells = layers * rows
    top = cells - rows
    planes = n // PLANE
    takers = 2 * PLANE
    me = lax.axis_index("gx")
    first, last = me == 0, me == n - 1
    zero_takes = lax.axis_index("groups") != 0
    taker = jnp.logical_and(me < takers, jnp.logical_or(me > 0, zero_takes))
    up, down = me + 1, me - 1

    def wait_rows(sem, row_count, wide=1):
        ref = pres.at[pl.ds(0, wide), pl.ds(0, row_count // wide)]
        pltpu.make_async_copy(ref, ref, sem).wait()

    def load(group, parts):
        for src, dst, begin, count in parts:
            at = pl.ds(begin, count)
            where = (at,) if len(src.shape) == 2 else (slice(None), at)
            pltpu.make_async_copy(src.at[where], dst.at[where], load_sem.at[group]).start()

    fields = [(pres_hbm, pres), (adj_hbm, adj)]
    others = [(perm_hbm, perm), (act_hbm, act), (code_hbm, code)]

    def span(refs, begin, end):
        return [(src, dst, begin, end - begin) for src, dst in refs]

    load(0, span(fields, 0, half) + span(fields, top + half, cells))
    load(1, span(fields, half, 2 * rows) + span(others, 0, 2 * rows))

    barrier = pltpu.get_barrier_semaphore()

    def greet(device):
        pl.semaphore_signal(barrier, inc=1, device_id={"gx": device}, device_id_type=MESH)

    @pl.when(jnp.logical_not(last))
    def _():
        greet(up)

    @pl.when(jnp.logical_not(first))
    def _():
        greet(down)

    @pl.when(taker)
    def _():
        def body(device, carry):
            @pl.when(device != me)
            def _():
                greet(device)

            return carry

        lax.fori_loop(0, n, body, 0)

    zero8 = jnp.zeros((8, rows), F32)
    for t in range(steps):
        pres[t, pl.ds(cells, 8), :] = zero8
        adj[t, pl.ds(cells, 8), :] = zero8
    for d in range(3):
        perm[d, pl.ds(cells, 8), :] = zero8
    act[pl.ds(cells, 8), :] = jnp.zeros((8, rows), jnp.int32)
    to_up_y[pl.ds(0, 8), :] = zero8

    low_a = pl.ds(0, half)
    top_b = pl.ds(top + half, half)

    def remote(src, dst, send, recv, device):
        return pltpu.make_async_remote_copy(
            src_ref=src, dst_ref=dst, send_sem=send, recv_sem=recv,
            device_id={"gx": device}, device_id_type=MESH,
        )

    goes_down = [
        remote(s, d, send_down, recv_down.at[int(i == 4)], down)
        for i, (s, d) in enumerate([
            (pres.at[:, low_a], above_pres),
            (adj.at[:, low_a], above_adj),
            (stage_perm, above_perm),
            (stage_low, above_log),
            (stage_rb, got_rb),
        ])
    ]
    goes_up = [
        remote(s, d, send_up, recv_up.at[int(i == 5)], up)
        for i, (s, d) in enumerate([
            (pres.at[:, top_b], below_pres),
            (adj.at[:, top_b], below_adj),
            (perm.at[0, top_b], below_perm),
            (stage_factor, below_factor),
            (stage_high, below_log),
            (stage_ra, got_ra),
        ])
    ]

    def start_up(*parts):
        @pl.when(jnp.logical_not(last))
        def _():
            for i in parts:
                goes_up[i].start()

    def start_down(*parts):
        @pl.when(jnp.logical_not(first))
        def _():
            for i in parts:
                goes_down[i].start()

    def one_if(condition):
        return jnp.where(condition, 1, 0)

    wait_rows(load_sem.at[0], 4 * steps * half, steps)
    pl.semaphore_wait(barrier, 1 + takers + one_if(zero_takes) - one_if(first) - one_if(last) - one_if(taker))
    start_up(0, 1)
    start_down(0, 1)

    load(2, span(fields + others, 2 * rows, 4 * rows))
    edge = 2 * steps * (2 * rows - half) + 7 * 2 * rows
    whole = (2 * steps + 7) * 2 * rows

    lane = lax.broadcasted_iota(jnp.int32, (BLOCK, rows), 1)
    sub = lax.broadcasted_iota(jnp.int32, (BLOCK, rows), 0)
    z_open = jnp.where(lane == rows - 1, 0.0, 1.0).astype(F32)

    def fold(square):
        return jnp.sum(square.reshape(square.shape[0] // 8, 8, rows), axis=0)

    def block(start, in_layer, acc, from_below, to_above):
        at = pl.ds(start, BLOCK)
        next_row = pl.ds(start + 1, BLOCK)
        next_layer = pl.ds(start + rows, BLOCK)
        px = py = pz = None
        for t in range(steps):
            p, a = pres[t, at, :], adj[t, at, :]
            y = (a - adj[t, next_row, :]) * (p - pres[t, next_row, :])
            z = (a - pltpu.roll(a, rows - 1, 1)) * (p - pltpu.roll(p, rows - 1, 1))
            py = y if t == 0 else py + y
            pz = z if t == 0 else pz + z
            if to_above:
                x = (a - adj[t, next_layer, :]) * (p - pres[t, next_layer, :])
                px = x if t == 0 else px + x
        opened = act[at, :].astype(F32)

        k = perm[2, at, :]
        factor = multiplier(code[2, at, :]) * opened * pltpu.roll(opened, rows - 1, 1) * z_open
        mine, above = face(pz, factor, k, pltpu.roll(k, rows - 1, 1))
        log = k * (mine + pltpu.roll(above, 1, 1))
        log_ref[2, at, :] = log
        acc = acc + fold(log * log)

        k = perm[1, at, :]
        y_open = jnp.where(in_layer + sub == rows - 1, 0.0, 1.0).astype(F32)
        factor = multiplier(code[1, at, :]) * opened * act[next_row, :].astype(F32) * y_open
        mine, above = face(py, factor, k, perm[1, next_row, :])
        to_up_y[next_row, :] = above
        log = k * (mine + to_up_y[at, :])
        log_ref[1, at, :] = log
        acc = acc + fold(log * log)

        k = perm[0, at, :]
        total = None
        if to_above:
            factor = multiplier(code[0, at, :]) * opened * act[next_layer, :].astype(F32)
            mine, above = face(px, factor, k, perm[0, next_layer, :])
            to_up_x[next_layer, :] = above
            total = mine
        if from_below:
            into = to_up_x[at, :]
            total = into if total is None else total + into
        log = k * total
        log_ref[0, at, :] = log
        if from_below and to_above:
            acc = acc + fold(log * log)
        return acc

    def layer_of(layer, acc, from_below=True, to_above=True):
        def body(i, acc):
            in_layer = pl.multiple_of(i * BLOCK, BLOCK)
            return block(pl.multiple_of(layer * rows + in_layer, BLOCK), in_layer, acc, from_below, to_above)

        return lax.fori_loop(0, rows // BLOCK, body, acc)

    def middle(begin, end, acc):
        return lax.fori_loop(begin, end, layer_of, acc)

    wait_rows(load_sem.at[1], edge, steps)
    load(3, span(fields + others, 4 * rows, 6 * rows))
    stage_perm[...] = perm[0, low_a, :] * act[low_a, :].astype(F32)
    acc = layer_of(0, jnp.zeros((8, rows), F32), from_below=False)
    start_down(2)
    stage_low[...] = log_ref[0, low_a, :]
    wait_rows(load_sem.at[2], whole, steps)
    load(4, span(fields, 6 * rows, top + half) + span(others, 6 * rows, cells))
    acc = middle(1, 3, acc)
    start_down(3)
    wait_rows(load_sem.at[3], whole, steps)
    acc = middle(3, 5, acc)
    wait_rows(load_sem.at[4], edge, steps)
    start_up(2)
    stage_factor[...] = multiplier(code[0, top_b, :]) * act[top_b, :].astype(F32)
    acc = middle(5, layers - 1, acc)
    start_up(3)
    stage_high[...] = perm[0, top_b, :] * to_up_x[top_b, :]
    acc = layer_of(layers - 1, acc, to_above=False)
    start_up(4)

    def products_of(lower_pres, lower_adj, lower_at, upper_pres, upper_adj, upper_at):
        total = None
        for t in range(steps):
            term = (lower_adj[t, lower_at, :] - upper_adj[t, upper_at, :]) * (
                lower_pres[t, lower_at, :] - upper_pres[t, upper_at, :]
            )
            total = term if t == 0 else total + term
        return total

    @pl.when(jnp.logical_not(last))
    def _():
        wait_rows(recv_down.at[0], (2 * steps + 2) * half, 2)

    @pl.when(jnp.logical_not(first))
    def _():
        wait_rows(recv_up.at[0], (2 * steps + 3) * half, 2)

    def keep(condition, value):
        return jnp.where(condition, value, 0.0)

    def shared(i, acc):
        there = pl.ds(pl.multiple_of(i * SHARED, SHARED), SHARED)
        here = pl.ds(pl.multiple_of(top + i * SHARED, SHARED), SHARED)
        inside = jnp.logical_not(last)
        products = products_of(pres, adj, here, above_pres, above_adj, there)
        factor = multiplier(code[0, here, :]) * act[here, :].astype(F32)
        k, k_up = perm[0, here, :], above_perm[there, :]
        mine, other = face(products, factor, k, k_up)
        log = log_ref[0, here, :] + keep(inside, k * mine)
        log_ref[0, here, :] = log
        reply = k_up * other
        stage_ra[there, :] = reply
        reply = keep(inside, reply + above_log[there, :])
        end = keep(last, log_ref[0, pl.ds(pl.multiple_of(top + half + i * SHARED, SHARED), SHARED), :])
        acc = acc + fold(log * log) + fold(reply * reply) + fold(end * end)

        here = pl.ds(pl.multiple_of(half + i * SHARED, SHARED), SHARED)
        inside = jnp.logical_not(first)
        products = products_of(below_pres, below_adj, there, pres, adj, here)
        factor = below_factor[there, :] * act[here, :].astype(F32)
        k, k_low = perm[0, here, :], below_perm[there, :]
        other, mine = face(products, factor, k_low, k)
        log = log_ref[0, here, :] + keep(inside, k * mine)
        log_ref[0, here, :] = log
        reply = k_low * other
        stage_rb[there, :] = reply
        reply = keep(inside, reply + below_log[there, :])
        end = keep(first, log_ref[0, there, :])
        return acc + fold(log * log) + fold(reply * reply) + fold(end * end)

    acc = lax.fori_loop(0, half // SHARED, shared, acc)

    partial = jnp.sum(acc, axis=0, keepdims=True)
    stage_sum[...] = partial
    to_takers = [remote(stage_sum, sums.at[me], send_sum.at[int(q == 0)], recv_sum, q) for q in range(takers)]
    to_zero = jnp.logical_and(zero_takes, jnp.logical_not(first))

    @pl.when(to_zero)
    def _():
        to_takers[0].start()

    @pl.when(jnp.logical_not(taker))
    def _():
        for copy in to_takers[1:]:
            copy.start()

    @pl.when(taker)
    def _():
        for q in range(1, takers):
            @pl.when(me != q)
            def _():
                to_takers[q].start()

    start_up(5)
    start_down(4)

    @pl.when(jnp.logical_not(first))
    def _():
        wait_rows(recv_up.at[1], half)
        log_ref[0, low_a, :] += got_ra[...]
        wait_rows(send_down, (2 * steps + 3) * half, 2)

    @pl.when(jnp.logical_not(last))
    def _():
        wait_rows(recv_down.at[1], half)
        log_ref[0, top_b, :] += got_rb[...]
        wait_rows(send_up, (2 * steps + 4) * half, 2)

    @pl.when(to_zero)
    def _():
        wait_rows(send_sum.at[1], 1)

    @pl.when(jnp.logical_and(taker, jnp.logical_not(first)))
    def _():
        wait_rows(send_sum.at[0], takers - 2)

    @pl.when(jnp.logical_or(first, jnp.logical_not(taker)))
    def _():
        wait_rows(send_sum.at[0], takers - 1)

    @pl.when(taker)
    def _():
        sums[me] = partial
        wait_rows(recv_sum, n - 1)
        quarter = n // 4
        total = sum(jnp.sum(sums[pl.ds(q * quarter, quarter)], axis=0) for q in range(4))
        total = jnp.sum(total, axis=1, keepdims=True)
        entries = 3 * cells * rows * n
        inverse = jnp.broadcast_to(1.0 / jnp.sqrt(total / entries + epsilon), inv_ref.shape)
        inv_ref[...] = inverse
        stage_inv[...] = inverse

        @pl.when(me >= PLANE)
        def _():
            for z in range(1, planes - 1):
                remote(stage_inv, got_inv, send_inv, recv_inv, me + z * PLANE).start()
            late = jnp.logical_and(me == takers - 1, jnp.logical_not(zero_takes))
            to_first = remote(stage_inv, got_inv, send_first, recv_inv, 0)

            @pl.when(late)
            def _():
                to_first.start()
                to_first.wait_send()

            wait_rows(send_inv, planes - 2)

    @pl.when(jnp.logical_not(taker))
    def _():
        wait_rows(recv_inv, 1)
        inv_ref[...] = got_inv[...]


def local(n, pressure, adjoint, permeability, active, fault_codes):
    steps, layers, rows, lanes = pressure.shape
    cells = layers * rows
    half = rows // 2
    planes = n // PLANE
    vmem, dma = pltpu.VMEM, pltpu.SemaphoreType.DMA
    halo = [
        vmem((steps, half, lanes), F32),
        vmem((steps, half, lanes), F32),
        vmem((half, lanes), F32),
    ]
    tile = vmem((half, lanes), F32)
    scratch = [
        vmem((steps, cells + 8, lanes), F32),
        vmem((steps, cells + 8, lanes), F32),
        vmem((3, cells + 8, lanes), F32),
        vmem((cells + 8, lanes), jnp.int32),
        vmem((3, cells, lanes), jnp.int32),
        vmem((cells, lanes), F32),
        vmem((cells + 8, lanes), F32),
        *halo, tile,
        *halo, tile, tile,
        tile, tile, tile, tile, tile, tile, tile, tile,
        vmem((1, lanes), F32), vmem((n, 1, lanes), F32),
        vmem((1, lanes), F32), vmem((1, lanes), F32),
        dma((5,)), dma, dma((2,)), dma, dma((2,)),
        dma((2,)), dma, dma, dma, dma,
    ]
    hbm = pl.BlockSpec(memory_space=pltpu.HBM)
    in_hbm = lambda x: pltpu.with_memory_space_constraint(x, pltpu.HBM)
    log, inverse = pl.pallas_call(
        functools.partial(kernel, steps, layers, rows, n),
        out_shape=(
            jax.ShapeDtypeStruct((3, cells, lanes), F32),
            jax.ShapeDtypeStruct((1, lanes), F32),
        ),
        in_specs=[hbm] * 5,
        out_specs=(pl.BlockSpec(memory_space=pltpu.VMEM), pl.BlockSpec(memory_space=pltpu.VMEM)),
        scratch_shapes=scratch,
        compiler_params=pltpu.CompilerParams(
            collective_id=0, has_side_effects=True, vmem_limit_bytes=32 * 1024 * 1024
        ),
        name="gradient",
    )(
        in_hbm(pressure.reshape(steps, cells, lanes)),
        in_hbm(adjoint.reshape(steps, cells, lanes)),
        in_hbm(permeability.reshape(3, cells, lanes)),
        in_hbm(active.reshape(cells, lanes)),
        in_hbm(fault_codes.reshape(3, cells, lanes)),
    )
    out = log * inverse[None]
    return out.reshape(3, layers, rows, lanes)


def solution(mesh):
    n = mesh.shape["gx"]
    whole = ("groups", "gx")
    four = P(None, whole, None, None)
    return jax.shard_map(
        functools.partial(local, n),
        mesh=mesh,
        in_specs=(four, four, four, P(whole, None, None), four),
        out_specs=four,
        check_vma=False,
    )
```

```python
import functools

import jax
import jax.numpy as jnp
from jax import lax
from jax.experimental import pallas as pl
from jax.experimental.pallas import tpu as pltpu
from jax.sharding import PartitionSpec as P

MESH = pl.DeviceIdType.MESH
F32 = jnp.float32

epsilon = 1e-06

PLANE = 8
BLOCK = 64

LOW = 56


def multiplier(codes):
    return jnp.where(codes == 0, 1.0, jnp.where(codes == 1, 0.6, jnp.where(codes == 2, 0.25, 0.05)))


def face(products, factor, lower_perm, upper_perm):
    inverse = 1.0 / (lower_perm + upper_perm)
    weight = (2.0 * factor) * products
    upper = upper_perm * inverse
    lower = lower_perm * inverse
    return weight * upper * upper, weight * lower * lower


def kernel(
    steps, layers, rows, n,
    pres_hbm, adj_hbm, perm_hbm, act_hbm, code_hbm,
    log_ref, inv_ref,
    pres, adj, perm, act, code,
    to_up_x, to_up_y,
    above_pres, above_adj, above_perm, above_log,
    below_pres, below_adj, below_perm, below_factor, below_log,
    stage_factor, stage_perm, stage_low, stage_high, stage_ra, stage_rb, got_ra, got_rb,
    stage_sum, sums, stage_inv, got_inv,
    load_sem, send_up, recv_up, send_down, recv_down,
    send_sum, recv_sum, send_inv, send_first, recv_inv,
):
    high = rows - LOW
    cells = layers * rows
    top = cells - rows
    planes = n // PLANE
    takers = 2 * PLANE
    me = lax.axis_index("gx")
    first, last = me == 0, me == n - 1
    zero_takes = lax.axis_index("groups") != 0
    taker = jnp.logical_and(me < takers, jnp.logical_or(me > 0, zero_takes))
    up, down = me + 1, me - 1

    def wait_rows(sem, row_count, wide=1):
        ref = pres.at[pl.ds(0, wide), pl.ds(0, row_count // wide)]
        pltpu.make_async_copy(ref, ref, sem).wait()

    def load(group, parts):
        for src, dst, begin, count in parts:
            at = pl.ds(begin, count)
            where = (at,) if len(src.shape) == 2 else (slice(None), at)
            pltpu.make_async_copy(src.at[where], dst.at[where], load_sem.at[group]).start()

    fields = [(pres_hbm, pres), (adj_hbm, adj)]
    others = [(perm_hbm, perm), (act_hbm, act), (code_hbm, code)]

    def span(refs, begin, end):
        return [(src, dst, begin, end - begin) for src, dst in refs]

    barrier = pltpu.get_barrier_semaphore()

    def greet(device):
        pl.semaphore_signal(barrier, inc=1, device_id={"gx": device}, device_id_type=MESH)

    @pl.when(jnp.logical_not(last))
    def _():
        greet(up)

    @pl.when(jnp.logical_not(first))
    def _():
        greet(down)

    load(0, span(fields, 0, LOW) + span(fields, top + LOW, cells))
    load(1, span(fields, LOW, 2 * rows) + span(others, 0, 2 * rows))

    @pl.when(taker)
    def _():
        def body(device, carry):
            @pl.when(device != me)
            def _():
                greet(device)

            return carry

        lax.fori_loop(0, n, body, 0)

    zero8 = jnp.zeros((8, rows), F32)
    for t in range(steps):
        pres[t, pl.ds(cells, 8), :] = zero8
        adj[t, pl.ds(cells, 8), :] = zero8
    for d in range(3):
        perm[d, pl.ds(cells, 8), :] = zero8
    act[pl.ds(cells, 8), :] = jnp.zeros((8, rows), jnp.int32)
    to_up_y[pl.ds(0, 8), :] = zero8

    low_a = pl.ds(0, LOW)
    top_b = pl.ds(top + LOW, high)

    def remote(src, dst, send, recv, device):
        return pltpu.make_async_remote_copy(
            src_ref=src, dst_ref=dst, send_sem=send, recv_sem=recv,
            device_id={"gx": device}, device_id_type=MESH,
        )

    goes_down = [
        remote(s, d, send_down, recv_down.at[int(i == 4)], down)
        for i, (s, d) in enumerate([
            (pres.at[:, low_a], above_pres),
            (adj.at[:, low_a], above_adj),
            (stage_perm, above_perm),
            (stage_low, above_log),
            (stage_rb, got_rb),
        ])
    ]
    goes_up = [
        remote(s, d, send_up, recv_up.at[int(i == 5)], up)
        for i, (s, d) in enumerate([
            (pres.at[:, top_b], below_pres),
            (adj.at[:, top_b], below_adj),
            (perm.at[0, top_b], below_perm),
            (stage_factor, below_factor),
            (stage_high, below_log),
            (stage_ra, got_ra),
        ])
    ]

    def start_up(*parts):
        @pl.when(jnp.logical_not(last))
        def _():
            for i in parts:
                goes_up[i].start()

    def start_down(*parts):
        @pl.when(jnp.logical_not(first))
        def _():
            for i in parts:
                goes_down[i].start()

    def one_if(condition):
        return jnp.where(condition, 1, 0)

    wait_rows(load_sem.at[0], 2 * steps * rows, steps)
    pl.semaphore_wait(barrier, 1 + takers + one_if(zero_takes) - one_if(first) - one_if(last) - one_if(taker))
    start_up(0, 1)
    start_down(0, 1)

    load(2, span(fields, 6 * rows, top + LOW) + span(others, 6 * rows, cells))
    first_two = 2 * steps * (2 * rows - LOW) + 7 * 2 * rows
    last_two = 2 * steps * (rows + LOW) + 7 * 2 * rows
    whole = (2 * steps + 7) * 2 * rows

    lane = lax.broadcasted_iota(jnp.int32, (BLOCK, rows), 1)
    sub = lax.broadcasted_iota(jnp.int32, (BLOCK, rows), 0)
    z_open = jnp.where(lane == rows - 1, 0.0, 1.0).astype(F32)

    def fold(square):
        return jnp.sum(square.reshape(square.shape[0] // 8, 8, rows), axis=0)

    def block(start, in_layer, acc, from_below, to_above):
        at = pl.ds(start, BLOCK)
        next_row = pl.ds(start + 1, BLOCK)
        next_layer = pl.ds(start + rows, BLOCK)
        px = py = pz = None
        for t in range(steps):
            p, a = pres[t, at, :], adj[t, at, :]
            y = (a - adj[t, next_row, :]) * (p - pres[t, next_row, :])
            z = (a - pltpu.roll(a, rows - 1, 1)) * (p - pltpu.roll(p, rows - 1, 1))
            py = y if t == 0 else py + y
            pz = z if t == 0 else pz + z
            if to_above:
                x = (a - adj[t, next_layer, :]) * (p - pres[t, next_layer, :])
                px = x if t == 0 else px + x
        opened = act[at, :].astype(F32)

        k = perm[2, at, :]
        factor = multiplier(code[2, at, :]) * opened * pltpu.roll(opened, rows - 1, 1) * z_open
        mine, above = face(pz, factor, k, pltpu.roll(k, rows - 1, 1))
        log = k * (mine + pltpu.roll(above, 1, 1))
        log_ref[2, at, :] = log
        acc = acc + fold(log * log)

        k = perm[1, at, :]
        y_open = jnp.where(in_layer + sub == rows - 1, 0.0, 1.0).astype(F32)
        factor = multiplier(code[1, at, :]) * opened * act[next_row, :].astype(F32) * y_open
        mine, above = face(py, factor, k, perm[1, next_row, :])
        to_up_y[next_row, :] = above
        log = k * (mine + to_up_y[at, :])
        log_ref[1, at, :] = log
        acc = acc + fold(log * log)

        k = perm[0, at, :]
        total = None
        if to_above:
            factor = multiplier(code[0, at, :]) * opened * act[next_layer, :].astype(F32)
            mine, above = face(px, factor, k, perm[0, next_layer, :])
            to_up_x[next_layer, :] = above
            total = mine
        if from_below:
            into = to_up_x[at, :]
            total = into if total is None else total + into
        log = k * total
        log_ref[0, at, :] = log
        if from_below and to_above:
            acc = acc + fold(log * log)
        return acc

    def layer_of(layer, acc, from_below=True, to_above=True):
        def body(i, acc):
            in_layer = pl.multiple_of(i * BLOCK, BLOCK)
            return block(pl.multiple_of(layer * rows + in_layer, BLOCK), in_layer, acc, from_below, to_above)

        return lax.fori_loop(0, rows // BLOCK, body, acc)

    def middle(begin, end, acc):
        return lax.fori_loop(begin, end, layer_of, acc)

    def products_of(lower_pres, lower_adj, lower_at, upper_pres, upper_adj, upper_at):
        total = None
        for t in range(steps):
            term = (lower_adj[t, lower_at, :] - upper_adj[t, upper_at, :]) * (
                lower_pres[t, lower_at, :] - upper_pres[t, upper_at, :]
            )
            total = term if t == 0 else total + term
        return total

    wait_rows(load_sem.at[1], first_two, steps)
    load(3, span(fields + others, 2 * rows, 4 * rows))
    stage_perm[...] = perm[0, low_a, :] * act[low_a, :].astype(F32)
    acc = layer_of(0, jnp.zeros((8, rows), F32), from_below=False)
    start_down(2)
    stage_low[...] = log_ref[0, low_a, :]

    wait_rows(load_sem.at[2], last_two, steps)
    load(4, span(fields + others, 4 * rows, 6 * rows))
    start_up(2)
    start_down(3)
    under = pl.ds(top - rows + LOW, high)
    products = products_of(pres, adj, under, pres, adj, top_b)
    opened = act[top_b, :].astype(F32)
    stage_factor[...] = multiplier(code[0, top_b, :]) * opened
    factor = multiplier(code[0, under, :]) * act[under, :].astype(F32) * opened
    stage_high[...] = perm[0, top_b, :] * face(products, factor, perm[0, under, :], perm[0, top_b, :])[1]

    wait_rows(load_sem.at[3], whole, steps)
    acc = layer_of(1, acc)
    start_up(3, 4)
    acc = layer_of(2, acc)
    wait_rows(load_sem.at[4], whole, steps)
    acc = middle(3, layers - 1, acc)
    acc = layer_of(layers - 1, acc, to_above=False)

    @pl.when(jnp.logical_not(last))
    def _():
        wait_rows(recv_down.at[0], (2 * steps + 2) * LOW, 2)

    @pl.when(jnp.logical_not(first))
    def _():
        wait_rows(recv_up.at[0], (2 * steps + 3) * high, 2)

    def keep(condition, value):
        return jnp.where(condition, value, 0.0)

    everything, here = pl.ds(0, LOW), pl.ds(top, LOW)
    inside = jnp.logical_not(last)
    products = products_of(pres, adj, here, above_pres, above_adj, everything)
    factor = multiplier(code[0, here, :]) * act[here, :].astype(F32)
    k, k_up = perm[0, here, :], above_perm[...]
    mine, other = face(products, factor, k, k_up)
    log = log_ref[0, here, :] + keep(inside, k * mine)
    log_ref[0, here, :] = log
    reply = k_up * other
    stage_ra[...] = reply
    reply = keep(inside, reply + above_log[...])
    end = keep(last, log_ref[0, top_b, :])
    acc = acc + fold(log * log) + fold(reply * reply) + fold(end * end)

    everything, here = pl.ds(0, high), pl.ds(LOW, high)
    inside = jnp.logical_not(first)
    products = products_of(below_pres, below_adj, everything, pres, adj, here)
    factor = below_factor[...] * act[here, :].astype(F32)
    k, k_low = perm[0, here, :], below_perm[...]
    other, mine = face(products, factor, k_low, k)
    log = log_ref[0, here, :] + keep(inside, k * mine)
    log_ref[0, here, :] = log
    reply = k_low * other
    stage_rb[...] = reply
    reply = keep(inside, reply + below_log[...])
    end = keep(first, log_ref[0, low_a, :])
    acc = acc + fold(log * log) + fold(reply * reply) + fold(end * end)

    partial = jnp.sum(acc, axis=0, keepdims=True)
    stage_sum[...] = partial
    to_takers = [remote(stage_sum, sums.at[me], send_sum.at[int(q == 0)], recv_sum, q) for q in range(takers)]
    to_zero = jnp.logical_and(zero_takes, jnp.logical_not(first))

    @pl.when(to_zero)
    def _():
        to_takers[0].start()

    @pl.when(jnp.logical_not(taker))
    def _():
        for copy in to_takers[1:]:
            copy.start()

    @pl.when(taker)
    def _():
        for q in range(1, takers):
            @pl.when(me != q)
            def _():
                to_takers[q].start()

    start_up(5)
    start_down(4)

    @pl.when(jnp.logical_not(first))
    def _():
        wait_rows(recv_up.at[1], LOW)
        log_ref[0, low_a, :] += got_ra[...]
        wait_rows(send_down, (2 * steps + 2) * LOW + high, 2)

    @pl.when(jnp.logical_not(last))
    def _():
        wait_rows(recv_down.at[1], high)
        log_ref[0, top_b, :] += got_rb[...]
        wait_rows(send_up, (2 * steps + 3) * high + LOW, 2)

    @pl.when(to_zero)
    def _():
        wait_rows(send_sum.at[1], 1)

    @pl.when(jnp.logical_and(taker, jnp.logical_not(first)))
    def _():
        wait_rows(send_sum.at[0], takers - 2)

    @pl.when(jnp.logical_or(first, jnp.logical_not(taker)))
    def _():
        wait_rows(send_sum.at[0], takers - 1)

    @pl.when(taker)
    def _():
        sums[me] = partial
        wait_rows(recv_sum, n - 1)
        quarter = n // 4
        total = sum(jnp.sum(sums[pl.ds(q * quarter, quarter)], axis=0) for q in range(4))
        total = jnp.sum(total, axis=1, keepdims=True)
        entries = 3 * cells * rows * n
        inverse = jnp.broadcast_to(1.0 / jnp.sqrt(total / entries + epsilon), inv_ref.shape)
        inv_ref[...] = inverse
        stage_inv[...] = inverse

        @pl.when(me >= PLANE)
        def _():
            for z in range(1, planes - 1):
                remote(stage_inv, got_inv, send_inv, recv_inv, me + z * PLANE).start()
            late = jnp.logical_and(me == takers - 1, jnp.logical_not(zero_takes))
            to_first = remote(stage_inv, got_inv, send_first, recv_inv, 0)

            @pl.when(late)
            def _():
                to_first.start()
                to_first.wait_send()

            wait_rows(send_inv, planes - 2)

    @pl.when(jnp.logical_not(taker))
    def _():
        wait_rows(recv_inv, 1)
        inv_ref[...] = got_inv[...]


def local(n, pressure, adjoint, permeability, active, fault_codes):
    steps, layers, rows, lanes = pressure.shape
    cells = layers * rows
    high = rows - LOW
    planes = n // PLANE
    vmem, dma = pltpu.VMEM, pltpu.SemaphoreType.DMA
    low_tile, high_tile = vmem((LOW, lanes), F32), vmem((high, lanes), F32)
    scratch = [
        vmem((steps, cells + 8, lanes), F32),
        vmem((steps, cells + 8, lanes), F32),
        vmem((3, cells + 8, lanes), F32),
        vmem((cells + 8, lanes), jnp.int32),
        vmem((3, cells, lanes), jnp.int32),
        vmem((cells, lanes), F32),
        vmem((cells + 8, lanes), F32),
        vmem((steps, LOW, lanes), F32), vmem((steps, LOW, lanes), F32), low_tile, low_tile,
        vmem((steps, high, lanes), F32), vmem((steps, high, lanes), F32), high_tile, high_tile, high_tile,
        high_tile, low_tile, low_tile, high_tile, low_tile, high_tile, low_tile, high_tile,
        vmem((1, lanes), F32), vmem((n, 1, lanes), F32),
        vmem((1, lanes), F32), vmem((1, lanes), F32),
        dma((5,)), dma, dma((2,)), dma, dma((2,)),
        dma((2,)), dma, dma, dma, dma,
    ]
    hbm = pl.BlockSpec(memory_space=pltpu.HBM)
    in_hbm = lambda x: pltpu.with_memory_space_constraint(x, pltpu.HBM)
    log, inverse = pl.pallas_call(
        functools.partial(kernel, steps, layers, rows, n),
        out_shape=(
            jax.ShapeDtypeStruct((3, cells, lanes), F32),
            jax.ShapeDtypeStruct((1, lanes), F32),
        ),
        in_specs=[hbm] * 5,
        out_specs=(pl.BlockSpec(memory_space=pltpu.VMEM), pl.BlockSpec(memory_space=pltpu.VMEM)),
        scratch_shapes=scratch,
        compiler_params=pltpu.CompilerParams(
            collective_id=0, has_side_effects=True, vmem_limit_bytes=32 * 1024 * 1024
        ),
        name="gradient",
    )(
        in_hbm(pressure.reshape(steps, cells, lanes)),
        in_hbm(adjoint.reshape(steps, cells, lanes)),
        in_hbm(permeability.reshape(3, cells, lanes)),
        in_hbm(active.reshape(cells, lanes)),
        in_hbm(fault_codes.reshape(3, cells, lanes)),
    )
    out = log * inverse[None]
    return out.reshape(3, layers, rows, lanes)


def solution(mesh):
    n = mesh.shape["gx"]
    whole = ("groups", "gx")
    four = P(None, whole, None, None)
    return jax.shard_map(
        functools.partial(local, n),
        mesh=mesh,
        in_specs=(four, four, four, P(whole, None, None), four),
        out_specs=four,
        check_vma=False,
    )
```

```python
import functools

import jax
import jax.numpy as jnp
from jax import lax
from jax.experimental import pallas as pl
from jax.experimental.pallas import tpu as pltpu
from jax.sharding import PartitionSpec as P

MESH = pl.DeviceIdType.MESH
F32 = jnp.float32

epsilon = 1e-06

PLANE = 8
BLOCK = 64

LOW = 56


def multiplier(codes):
    return jnp.where(codes == 0, 1.0, jnp.where(codes == 1, 0.6, jnp.where(codes == 2, 0.25, 0.05)))


def face(products, factor, lower_perm, upper_perm):
    inverse = 1.0 / (lower_perm + upper_perm)
    weight = (2.0 * factor) * products
    upper = upper_perm * inverse
    lower = lower_perm * inverse
    return weight * upper * upper, weight * lower * lower


def kernel(
    steps, layers, rows, n,
    pres_hbm, adj_hbm, perm_hbm, act_hbm, code_hbm,
    log_ref, inv_ref,
    both, perm, act, code,
    to_up_x, to_up_y,
    above_both, above_rest, below_both, below_rest,
    stage_down, stage_up, stage_ra, stage_rb, got_ra, got_rb,
    stage_sum, sums, stage_inv, got_inv,
    load_sem, send_up, recv_up, send_down, recv_down,
    send_sum, recv_sum, send_inv, send_first, recv_inv,
):
    high = rows - LOW

    def halves(ref):
        return ref.at[pl.ds(0, steps)], ref.at[pl.ds(steps, steps)]

    pres, adj = halves(both)
    above_pres, above_adj = halves(above_both)
    below_pres, below_adj = halves(below_both)
    above_perm, above_log = above_rest.at[0], above_rest.at[1]
    below_perm, below_factor, below_log = (below_rest.at[i] for i in range(3))
    cells = layers * rows
    top = cells - rows
    planes = n // PLANE
    takers = 2 * PLANE
    me = lax.axis_index("gx")
    first, last = me == 0, me == n - 1
    zero_takes = lax.axis_index("groups") != 0
    taker = jnp.logical_and(me < takers, jnp.logical_or(me > 0, zero_takes))
    up, down = me + 1, me - 1

    def wait_rows(sem, row_count, wide=1):
        ref = both.at[pl.ds(0, wide), pl.ds(0, row_count // wide)]
        pltpu.make_async_copy(ref, ref, sem).wait()

    def load(group, parts):
        for src, dst, begin, count in parts:
            at = pl.ds(begin, count)
            where = (at,) if len(src.shape) == 2 else (slice(None), at)
            pltpu.make_async_copy(src.at[where], dst.at[where], load_sem.at[group]).start()

    fields = [(pres_hbm, pres), (adj_hbm, adj)]
    others = [(perm_hbm, perm), (act_hbm, act), (code_hbm, code)]

    def span(refs, begin, end):
        return [(src, dst, begin, end - begin) for src, dst in refs]

    load(0, span(fields, top + LOW, cells))
    load(5, span(fields, 0, LOW))
    load(1, span(fields, LOW, 2 * rows) + span(others, 0, 2 * rows))

    barrier = pltpu.get_barrier_semaphore()

    def greet(device):
        pl.semaphore_signal(barrier, inc=1, device_id={"gx": device}, device_id_type=MESH)

    @pl.when(jnp.logical_not(last))
    def _():
        greet(up)

    @pl.when(jnp.logical_not(first))
    def _():
        greet(down)

    @pl.when(taker)
    def _():
        def body(device, carry):
            @pl.when(device != me)
            def _():
                greet(device)

            return carry

        lax.fori_loop(0, n, body, 0)

    zero8 = jnp.zeros((8, rows), F32)
    for t in range(steps):
        pres[t, pl.ds(cells, 8), :] = zero8
        adj[t, pl.ds(cells, 8), :] = zero8
    for d in range(3):
        perm[d, pl.ds(cells, 8), :] = zero8
    act[pl.ds(cells, 8), :] = jnp.zeros((8, rows), jnp.int32)
    to_up_y[pl.ds(0, 8), :] = zero8

    low_a = pl.ds(0, LOW)
    top_b = pl.ds(top + LOW, high)

    def remote(src, dst, send, recv, device):
        return pltpu.make_async_remote_copy(
            src_ref=src, dst_ref=dst, send_sem=send, recv_sem=recv,
            device_id={"gx": device}, device_id_type=MESH,
        )

    goes_down = [
        remote(s, d, send_down, recv_down.at[int(i == 2)], down)
        for i, (s, d) in enumerate([(both.at[:, low_a], above_both), (stage_down, above_rest), (stage_rb, got_rb)])
    ]
    goes_up = [
        remote(s, d, send_up, recv_up.at[int(i == 2)], up)
        for i, (s, d) in enumerate([(both.at[:, top_b], below_both), (stage_up, below_rest), (stage_ra, got_ra)])
    ]

    def start_up(*parts):
        @pl.when(jnp.logical_not(last))
        def _():
            for i in parts:
                goes_up[i].start()

    def start_down(*parts):
        @pl.when(jnp.logical_not(first))
        def _():
            for i in parts:
                goes_down[i].start()

    def one_if(condition):
        return jnp.where(condition, 1, 0)

    wait_rows(load_sem.at[0], 2 * steps * high, steps)
    pl.semaphore_wait(barrier, 1 + takers + one_if(zero_takes) - one_if(first) - one_if(last) - one_if(taker))
    start_up(0)
    wait_rows(load_sem.at[5], 2 * steps * LOW, steps)
    start_down(0)

    load(2, span(fields, 6 * rows, top + LOW) + span(others, 6 * rows, cells))
    first_two = 2 * steps * (2 * rows - LOW) + 7 * 2 * rows
    last_two = 2 * steps * (rows + LOW) + 7 * 2 * rows
    whole = (2 * steps + 7) * 2 * rows

    lane = lax.broadcasted_iota(jnp.int32, (BLOCK, rows), 1)
    sub = lax.broadcasted_iota(jnp.int32, (BLOCK, rows), 0)
    z_open = jnp.where(lane == rows - 1, 0.0, 1.0).astype(F32)

    def fold(square):
        return jnp.sum(square.reshape(square.shape[0] // 8, 8, rows), axis=0)

    def block(start, in_layer, acc, from_below, to_above):
        at = pl.ds(start, BLOCK)
        next_row = pl.ds(start + 1, BLOCK)
        next_layer = pl.ds(start + rows, BLOCK)
        px = py = pz = None
        for t in range(steps):
            p, a = pres[t, at, :], adj[t, at, :]
            y = (a - adj[t, next_row, :]) * (p - pres[t, next_row, :])
            z = (a - pltpu.roll(a, rows - 1, 1)) * (p - pltpu.roll(p, rows - 1, 1))
            py = y if t == 0 else py + y
            pz = z if t == 0 else pz + z
            if to_above:
                x = (a - adj[t, next_layer, :]) * (p - pres[t, next_layer, :])
                px = x if t == 0 else px + x
        opened = act[at, :].astype(F32)

        k = perm[2, at, :]
        factor = multiplier(code[2, at, :]) * opened * pltpu.roll(opened, rows - 1, 1) * z_open
        mine, above = face(pz, factor, k, pltpu.roll(k, rows - 1, 1))
        log = k * (mine + pltpu.roll(above, 1, 1))
        log_ref[2, at, :] = log
        acc = acc + fold(log * log)

        k = perm[1, at, :]
        y_open = jnp.where(in_layer + sub == rows - 1, 0.0, 1.0).astype(F32)
        factor = multiplier(code[1, at, :]) * opened * act[next_row, :].astype(F32) * y_open
        mine, above = face(py, factor, k, perm[1, next_row, :])
        to_up_y[next_row, :] = above
        log = k * (mine + to_up_y[at, :])
        log_ref[1, at, :] = log
        acc = acc + fold(log * log)

        k = perm[0, at, :]
        total = None
        if to_above:
            factor = multiplier(code[0, at, :]) * opened * act[next_layer, :].astype(F32)
            mine, above = face(px, factor, k, perm[0, next_layer, :])
            to_up_x[next_layer, :] = above
            total = mine
        if from_below:
            into = to_up_x[at, :]
            total = into if total is None else total + into
        log = k * total
        log_ref[0, at, :] = log
        if from_below and to_above:
            acc = acc + fold(log * log)
        return acc

    def layer_of(layer, acc, from_below=True, to_above=True):
        def body(i, acc):
            in_layer = pl.multiple_of(i * BLOCK, BLOCK)
            return block(pl.multiple_of(layer * rows + in_layer, BLOCK), in_layer, acc, from_below, to_above)

        return lax.fori_loop(0, rows // BLOCK, body, acc)

    def middle(begin, end, acc):
        return lax.fori_loop(begin, end, layer_of, acc)

    def products_of(lower_pres, lower_adj, lower_at, upper_pres, upper_adj, upper_at):
        total = None
        for t in range(steps):
            term = (lower_adj[t, lower_at, :] - upper_adj[t, upper_at, :]) * (
                lower_pres[t, lower_at, :] - upper_pres[t, upper_at, :]
            )
            total = term if t == 0 else total + term
        return total

    wait_rows(load_sem.at[1], first_two, steps)
    load(3, span(fields + others, 2 * rows, 4 * rows))
    stage_down[0] = perm[0, low_a, :] * act[low_a, :].astype(F32)
    acc = layer_of(0, jnp.zeros((8, rows), F32), from_below=False)
    stage_down[1] = log_ref[0, low_a, :]

    wait_rows(load_sem.at[2], last_two, steps)
    load(4, span(fields + others, 4 * rows, 6 * rows))
    start_down(1)
    stage_up[0] = perm[0, top_b, :]
    under = pl.ds(top - rows + LOW, high)
    products = products_of(pres, adj, under, pres, adj, top_b)
    opened = act[top_b, :].astype(F32)
    stage_up[1] = multiplier(code[0, top_b, :]) * opened
    factor = multiplier(code[0, under, :]) * act[under, :].astype(F32) * opened
    stage_up[2] = perm[0, top_b, :] * face(products, factor, perm[0, under, :], perm[0, top_b, :])[1]

    wait_rows(load_sem.at[3], whole, steps)
    acc = layer_of(1, acc)
    start_up(1)
    acc = layer_of(2, acc)
    wait_rows(load_sem.at[4], whole, steps)
    acc = middle(3, layers - 1, acc)
    acc = layer_of(layers - 1, acc, to_above=False)

    @pl.when(jnp.logical_not(last))
    def _():
        wait_rows(recv_down.at[0], (2 * steps + 2) * LOW, 2)

    def keep(condition, value):
        return jnp.where(condition, value, 0.0)

    everything, here = pl.ds(0, LOW), pl.ds(top, LOW)
    inside = jnp.logical_not(last)
    products = products_of(pres, adj, here, above_pres, above_adj, everything)
    factor = multiplier(code[0, here, :]) * act[here, :].astype(F32)
    k, k_up = perm[0, here, :], above_perm[...]
    mine, other = face(products, factor, k, k_up)
    log = log_ref[0, here, :] + keep(inside, k * mine)
    log_ref[0, here, :] = log
    reply = k_up * other
    stage_ra[...] = reply
    reply = keep(inside, reply + above_log[...])
    end = keep(last, log_ref[0, top_b, :])
    acc = acc + fold(log * log) + fold(reply * reply) + fold(end * end)

    @pl.when(jnp.logical_not(first))
    def _():
        wait_rows(recv_up.at[0], (2 * steps + 3) * high, 2)

    everything, here = pl.ds(0, high), pl.ds(LOW, high)
    inside = jnp.logical_not(first)
    products = products_of(below_pres, below_adj, everything, pres, adj, here)
    factor = below_factor[...] * act[here, :].astype(F32)
    k, k_low = perm[0, here, :], below_perm[...]
    other, mine = face(products, factor, k_low, k)
    log = log_ref[0, here, :] + keep(inside, k * mine)
    log_ref[0, here, :] = log
    reply = k_low * other
    stage_rb[...] = reply
    reply = keep(inside, reply + below_log[...])
    end = keep(first, log_ref[0, low_a, :])
    acc = acc + fold(log * log) + fold(reply * reply) + fold(end * end)

    partial = jnp.sum(acc, axis=0, keepdims=True)
    stage_sum[...] = partial
    to_takers = [remote(stage_sum, sums.at[me], send_sum.at[int(q == 0)], recv_sum, q) for q in range(takers)]
    to_zero = jnp.logical_and(zero_takes, jnp.logical_not(first))

    @pl.when(to_zero)
    def _():
        to_takers[0].start()

    @pl.when(jnp.logical_not(taker))
    def _():
        for copy in to_takers[1:]:
            copy.start()

    @pl.when(taker)
    def _():
        for q in range(1, takers):
            @pl.when(me != q)
            def _():
                to_takers[q].start()

    start_up(2)
    start_down(2)

    @pl.when(jnp.logical_not(first))
    def _():
        wait_rows(recv_up.at[1], LOW)
        log_ref[0, low_a, :] += got_ra[...]
        wait_rows(send_down, (2 * steps + 2) * LOW + high, 2)

    @pl.when(jnp.logical_not(last))
    def _():
        wait_rows(recv_down.at[1], high)
        log_ref[0, top_b, :] += got_rb[...]
        wait_rows(send_up, (2 * steps + 3) * high + LOW, 2)

    @pl.when(to_zero)
    def _():
        wait_rows(send_sum.at[1], 1)

    @pl.when(jnp.logical_and(taker, jnp.logical_not(first)))
    def _():
        wait_rows(send_sum.at[0], takers - 2)

    @pl.when(jnp.logical_or(first, jnp.logical_not(taker)))
    def _():
        wait_rows(send_sum.at[0], takers - 1)

    @pl.when(taker)
    def _():
        sums[me] = partial
        wait_rows(recv_sum, n - 1)
        quarter = n // 4
        total = sum(jnp.sum(sums[pl.ds(q * quarter, quarter)], axis=0) for q in range(4))
        total = jnp.sum(total, axis=1, keepdims=True)
        entries = 3 * cells * rows * n
        inverse = jnp.broadcast_to(1.0 / jnp.sqrt(total / entries + epsilon), inv_ref.shape)
        inv_ref[...] = inverse
        stage_inv[...] = inverse

        @pl.when(me >= PLANE)
        def _():
            for z in range(1, planes - 1):
                remote(stage_inv, got_inv, send_inv, recv_inv, me + z * PLANE).start()
            late = jnp.logical_and(me == takers - 1, jnp.logical_not(zero_takes))
            to_first = remote(stage_inv, got_inv, send_first, recv_inv, 0)

            @pl.when(late)
            def _():
                to_first.start()
                to_first.wait_send()

            wait_rows(send_inv, planes - 2)

    @pl.when(jnp.logical_not(taker))
    def _():
        wait_rows(recv_inv, 1)
        inv_ref[...] = got_inv[...]


def local(n, pressure, adjoint, permeability, active, fault_codes):
    steps, layers, rows, lanes = pressure.shape
    cells = layers * rows
    high = rows - LOW
    planes = n // PLANE
    vmem, dma = pltpu.VMEM, pltpu.SemaphoreType.DMA
    low_tile, high_tile = vmem((LOW, lanes), F32), vmem((high, lanes), F32)
    scratch = [
        vmem((2 * steps, cells + 8, lanes), F32),
        vmem((3, cells + 8, lanes), F32),
        vmem((cells + 8, lanes), jnp.int32),
        vmem((3, cells, lanes), jnp.int32),
        vmem((cells, lanes), F32),
        vmem((cells + 8, lanes), F32),
        vmem((2 * steps, LOW, lanes), F32), vmem((2, LOW, lanes), F32),
        vmem((2 * steps, high, lanes), F32), vmem((3, high, lanes), F32),
        vmem((2, LOW, lanes), F32), vmem((3, high, lanes), F32),
        low_tile, high_tile, low_tile, high_tile,
        vmem((1, lanes), F32), vmem((n, 1, lanes), F32),
        vmem((1, lanes), F32), vmem((1, lanes), F32),
        dma((6,)), dma, dma((2,)), dma, dma((2,)),
        dma((2,)), dma, dma, dma, dma,
    ]
    hbm = pl.BlockSpec(memory_space=pltpu.HBM)
    in_hbm = lambda x: pltpu.with_memory_space_constraint(x, pltpu.HBM)
    log, inverse = pl.pallas_call(
        functools.partial(kernel, steps, layers, rows, n),
        out_shape=(
            jax.ShapeDtypeStruct((3, cells, lanes), F32),
            jax.ShapeDtypeStruct((1, lanes), F32),
        ),
        in_specs=[hbm] * 5,
        out_specs=(pl.BlockSpec(memory_space=pltpu.VMEM), pl.BlockSpec(memory_space=pltpu.VMEM)),
        scratch_shapes=scratch,
        compiler_params=pltpu.CompilerParams(
            collective_id=0, has_side_effects=True, vmem_limit_bytes=32 * 1024 * 1024
        ),
        name="gradient",
    )(
        in_hbm(pressure.reshape(steps, cells, lanes)),
        in_hbm(adjoint.reshape(steps, cells, lanes)),
        in_hbm(permeability.reshape(3, cells, lanes)),
        in_hbm(active.reshape(cells, lanes)),
        in_hbm(fault_codes.reshape(3, cells, lanes)),
    )
    out = log * inverse[None]
    return out.reshape(3, layers, rows, lanes)


def solution(mesh):
    n = mesh.shape["gx"]
    whole = ("groups", "gx")
    four = P(None, whole, None, None)
    return jax.shard_map(
        functools.partial(local, n),
        mesh=mesh,
        in_specs=(four, four, four, P(whole, None, None), four),
        out_specs=four,
        check_vma=False,
    )
```

```python
import functools

import jax
import jax.numpy as jnp
from jax import lax
from jax.experimental import pallas as pl
from jax.experimental.pallas import tpu as pltpu
from jax.sharding import PartitionSpec as P

MESH = pl.DeviceIdType.MESH
F32 = jnp.float32

epsilon = 1e-06

PLANE = 8
BLOCK = 64

LOW = 56

PIECES = 6


def multiplier(codes):
    return jnp.where(codes == 0, 1.0, jnp.where(codes == 1, 0.6, jnp.where(codes == 2, 0.25, 0.05)))


def face(products, factor, lower_perm, upper_perm):
    inverse = 1.0 / (lower_perm + upper_perm)
    weight = (2.0 * factor) * products
    upper = upper_perm * inverse
    lower = lower_perm * inverse
    return weight * upper * upper, weight * lower * lower


def kernel(
    steps, layers, rows, n,
    pres_hbm, adj_hbm, perm_hbm, act_hbm, code_hbm,
    log_ref, inv_ref,
    both, perm, act, code,
    to_up_x, to_up_y,
    above_both, above_rest, below_both, below_rest,
    stage_down, stage_up, stage_ra, stage_rb, got_ra, got_rb,
    stage_sum, sums, stage_inv, got_inv,
    load_sem, send_up, recv_up, send_down, recv_down,
    send_sum, recv_sum, send_inv, send_first, recv_inv,
):
    high = rows - LOW

    def halves(ref):
        return ref.at[pl.ds(0, steps)], ref.at[pl.ds(steps, steps)]

    pres, adj = halves(both)
    above_pres, above_adj = halves(above_both)
    below_pres, below_adj = halves(below_both)
    above_perm, above_log = above_rest.at[0], above_rest.at[1]
    below_perm, below_factor, below_log = (below_rest.at[i] for i in range(3))
    cells = layers * rows
    top = cells - rows
    planes = n // PLANE
    takers = 2 * PLANE
    me = lax.axis_index("gx")
    first, last = me == 0, me == n - 1
    zero_takes = lax.axis_index("groups") != 0
    taker = jnp.logical_and(me < takers, jnp.logical_or(me > 0, zero_takes))
    up, down = me + 1, me - 1

    def wait_rows(sem, row_count, wide=1):
        ref = both.at[pl.ds(0, wide), pl.ds(0, row_count // wide)]
        pltpu.make_async_copy(ref, ref, sem).wait()

    def load(group, parts):
        for src, dst, begin, count in parts:
            at = pl.ds(begin, count)
            where = (at,) if len(src.shape) == 2 else (slice(None), at)
            pltpu.make_async_copy(src.at[where], dst.at[where], load_sem.at[group]).start()

    fields = [(pres_hbm, pres), (adj_hbm, adj)]
    others = [(perm_hbm, perm), (act_hbm, act), (code_hbm, code)]

    def span(refs, begin, end):
        return [(src, dst, begin, end - begin) for src, dst in refs]

    load(0, span(fields, top + LOW, cells))
    load(5, span(fields, 0, LOW))
    load(1, span(fields, LOW, 2 * rows) + span(others, 0, 2 * rows))

    barrier = pltpu.get_barrier_semaphore()

    def greet(device):
        pl.semaphore_signal(barrier, inc=1, device_id={"gx": device}, device_id_type=MESH)

    @pl.when(jnp.logical_not(last))
    def _():
        greet(up)

    @pl.when(jnp.logical_not(first))
    def _():
        greet(down)

    @pl.when(taker)
    def _():
        def body(device, carry):
            @pl.when(device != me)
            def _():
                greet(device)

            return carry

        lax.fori_loop(0, n, body, 0)

    zero8 = jnp.zeros((8, rows), F32)
    for t in range(steps):
        pres[t, pl.ds(cells, 8), :] = zero8
        adj[t, pl.ds(cells, 8), :] = zero8
    for d in range(3):
        perm[d, pl.ds(cells, 8), :] = zero8
    act[pl.ds(cells, 8), :] = jnp.zeros((8, rows), jnp.int32)
    to_up_y[pl.ds(0, 8), :] = zero8

    low_a = pl.ds(0, LOW)
    top_b = pl.ds(top + LOW, high)

    def remote(src, dst, send, recv, device):
        return pltpu.make_async_remote_copy(
            src_ref=src, dst_ref=dst, send_sem=send, recv_sem=recv,
            device_id={"gx": device}, device_id_type=MESH,
        )

    goes_down = [
        remote(s, d, send_down, recv_down.at[int(i == 2)], down)
        for i, (s, d) in enumerate([(both.at[:, low_a], above_both), (stage_down, above_rest), (stage_rb, got_rb)])
    ]
    goes_up = [
        remote(s, d, send_up, recv_up.at[int(i == 2)], up)
        for i, (s, d) in enumerate([(both.at[:, top_b], below_both), (stage_up, below_rest), (stage_ra, got_ra)])
    ]

    def start_up(*parts):
        @pl.when(jnp.logical_not(last))
        def _():
            for i in parts:
                goes_up[i].start()

    def start_down(*parts):
        @pl.when(jnp.logical_not(first))
        def _():
            for i in parts:
                goes_down[i].start()

    def one_if(condition):
        return jnp.where(condition, 1, 0)

    wait_rows(load_sem.at[0], 2 * steps * high, steps)
    pl.semaphore_wait(barrier, 1 + takers + one_if(zero_takes) - one_if(first) - one_if(last) - one_if(taker))
    start_up(0)
    wait_rows(load_sem.at[5], 2 * steps * LOW, steps)
    start_down(0)

    load(2, span(fields, 6 * rows, top + LOW) + span(others, 6 * rows, cells))
    first_two = 2 * steps * (2 * rows - LOW) + 7 * 2 * rows
    last_two = 2 * steps * (rows + LOW) + 7 * 2 * rows
    whole = (2 * steps + 7) * 2 * rows

    lane = lax.broadcasted_iota(jnp.int32, (BLOCK, rows), 1)
    sub = lax.broadcasted_iota(jnp.int32, (BLOCK, rows), 0)
    z_open = jnp.where(lane == rows - 1, 0.0, 1.0).astype(F32)

    def fold(square):
        return jnp.sum(square.reshape(square.shape[0] // 8, 8, rows), axis=0)

    def block(start, in_layer, acc, from_below, to_above):
        at = pl.ds(start, BLOCK)
        next_row = pl.ds(start + 1, BLOCK)
        next_layer = pl.ds(start + rows, BLOCK)
        px = py = pz = None
        for t in range(steps):
            p, a = pres[t, at, :], adj[t, at, :]
            y = (a - adj[t, next_row, :]) * (p - pres[t, next_row, :])
            z = (a - pltpu.roll(a, rows - 1, 1)) * (p - pltpu.roll(p, rows - 1, 1))
            py = y if t == 0 else py + y
            pz = z if t == 0 else pz + z
            if to_above:
                x = (a - adj[t, next_layer, :]) * (p - pres[t, next_layer, :])
                px = x if t == 0 else px + x
        opened = act[at, :].astype(F32)

        k = perm[2, at, :]
        factor = multiplier(code[2, at, :]) * opened * pltpu.roll(opened, rows - 1, 1) * z_open
        mine, above = face(pz, factor, k, pltpu.roll(k, rows - 1, 1))
        log = k * (mine + pltpu.roll(above, 1, 1))
        log_ref[2, at, :] = log
        acc = acc + fold(log * log)

        k = perm[1, at, :]
        y_open = jnp.where(in_layer + sub == rows - 1, 0.0, 1.0).astype(F32)
        factor = multiplier(code[1, at, :]) * opened * act[next_row, :].astype(F32) * y_open
        mine, above = face(py, factor, k, perm[1, next_row, :])
        to_up_y[next_row, :] = above
        log = k * (mine + to_up_y[at, :])
        log_ref[1, at, :] = log
        acc = acc + fold(log * log)

        k = perm[0, at, :]
        total = None
        if to_above:
            factor = multiplier(code[0, at, :]) * opened * act[next_layer, :].astype(F32)
            mine, above = face(px, factor, k, perm[0, next_layer, :])
            to_up_x[next_layer, :] = above
            total = mine
        if from_below:
            into = to_up_x[at, :]
            total = into if total is None else total + into
        log = k * total
        log_ref[0, at, :] = log
        if from_below and to_above:
            acc = acc + fold(log * log)
        return acc

    def layer_of(layer, acc, from_below=True, to_above=True):
        def body(i, acc):
            in_layer = pl.multiple_of(i * BLOCK, BLOCK)
            return block(pl.multiple_of(layer * rows + in_layer, BLOCK), in_layer, acc, from_below, to_above)

        return lax.fori_loop(0, rows // BLOCK, body, acc)

    def middle(begin, end, acc):
        return lax.fori_loop(begin, end, layer_of, acc)

    def products_of(lower_pres, lower_adj, lower_at, upper_pres, upper_adj, upper_at):
        total = None
        for t in range(steps):
            term = (lower_adj[t, lower_at, :] - upper_adj[t, upper_at, :]) * (
                lower_pres[t, lower_at, :] - upper_pres[t, upper_at, :]
            )
            total = term if t == 0 else total + term
        return total

    wait_rows(load_sem.at[1], first_two, steps)
    load(3, span(fields + others, 2 * rows, 4 * rows))
    stage_down[0] = perm[0, low_a, :] * act[low_a, :].astype(F32)
    acc = layer_of(0, jnp.zeros((8, rows), F32), from_below=False)
    stage_down[1] = log_ref[0, low_a, :]

    wait_rows(load_sem.at[2], last_two, steps)
    load(4, span(fields + others, 4 * rows, 6 * rows))
    start_down(1)
    stage_up[0] = perm[0, top_b, :]
    under = pl.ds(top - rows + LOW, high)
    products = products_of(pres, adj, under, pres, adj, top_b)
    opened = act[top_b, :].astype(F32)
    stage_up[1] = multiplier(code[0, top_b, :]) * opened
    factor = multiplier(code[0, under, :]) * act[under, :].astype(F32) * opened
    stage_up[2] = perm[0, top_b, :] * face(products, factor, perm[0, under, :], perm[0, top_b, :])[1]

    wait_rows(load_sem.at[3], whole, steps)
    acc = layer_of(1, acc)
    start_up(1)
    acc = layer_of(2, acc)
    wait_rows(load_sem.at[4], whole, steps)
    acc = middle(3, layers - 1, acc)
    acc = layer_of(layers - 1, acc, to_above=False)

    @pl.when(jnp.logical_not(last))
    def _():
        wait_rows(recv_down.at[0], (2 * steps + 2) * LOW, 2)

    def keep(condition, value):
        return jnp.where(condition, value, 0.0)

    everything, here = pl.ds(0, LOW), pl.ds(top, LOW)
    inside = jnp.logical_not(last)
    products = products_of(pres, adj, here, above_pres, above_adj, everything)
    factor = multiplier(code[0, here, :]) * act[here, :].astype(F32)
    k, k_up = perm[0, here, :], above_perm[...]
    mine, other = face(products, factor, k, k_up)
    log = log_ref[0, here, :] + keep(inside, k * mine)
    log_ref[0, here, :] = log
    reply = k_up * other
    stage_ra[...] = reply
    reply = keep(inside, reply + above_log[...])
    end = keep(last, log_ref[0, top_b, :])
    acc = acc + fold(log * log) + fold(reply * reply) + fold(end * end)

    @pl.when(jnp.logical_not(first))
    def _():
        wait_rows(recv_up.at[0], (2 * steps + 3) * high, 2)

    everything, here = pl.ds(0, high), pl.ds(LOW, high)
    inside = jnp.logical_not(first)
    products = products_of(below_pres, below_adj, everything, pres, adj, here)
    factor = below_factor[...] * act[here, :].astype(F32)
    k, k_low = perm[0, here, :], below_perm[...]
    other, mine = face(products, factor, k_low, k)
    log = log_ref[0, here, :] + keep(inside, k * mine)
    log_ref[0, here, :] = log
    reply = k_low * other
    stage_rb[...] = reply
    reply = keep(inside, reply + below_log[...])
    end = keep(first, log_ref[0, low_a, :])
    acc = acc + fold(log * log) + fold(reply * reply) + fold(end * end)

    partial = jnp.sum(acc, axis=0, keepdims=True)
    stage_sum[...] = partial
    to_takers = [remote(stage_sum, sums.at[me], send_sum.at[int(q == 0)], recv_sum, q) for q in range(takers)]
    to_zero = jnp.logical_and(zero_takes, jnp.logical_not(first))

    @pl.when(to_zero)
    def _():
        to_takers[0].start()

    @pl.when(jnp.logical_not(taker))
    def _():
        for copy in to_takers[1:]:
            copy.start()

    @pl.when(taker)
    def _():
        for q in range(1, takers):
            @pl.when(me != q)
            def _():
                to_takers[q].start()

    start_up(2)
    start_down(2)

    @pl.when(jnp.logical_not(first))
    def _():
        wait_rows(recv_up.at[1], LOW)
        log_ref[0, low_a, :] += got_ra[...]
        wait_rows(send_down, (2 * steps + 2) * LOW + high, 2)

    @pl.when(jnp.logical_not(last))
    def _():
        wait_rows(recv_down.at[1], high)
        log_ref[0, top_b, :] += got_rb[...]
        wait_rows(send_up, (2 * steps + 3) * high + LOW, 2)

    @pl.when(to_zero)
    def _():
        wait_rows(send_sum.at[1], 1)

    @pl.when(jnp.logical_and(taker, jnp.logical_not(first)))
    def _():
        wait_rows(send_sum.at[0], takers - 2)

    @pl.when(jnp.logical_or(first, jnp.logical_not(taker)))
    def _():
        wait_rows(send_sum.at[0], takers - 1)

    @pl.when(taker)
    def _():
        sums[me] = partial
        wait_rows(recv_sum, n - 1)
        quarter = n // 4
        total = sum(jnp.sum(sums[pl.ds(q * quarter, quarter)], axis=0) for q in range(4))
        total = jnp.sum(total, axis=1, keepdims=True)
        entries = 3 * cells * rows * n
        inverse = jnp.broadcast_to(1.0 / jnp.sqrt(total / entries + epsilon), inv_ref.shape)
        inv_ref[...] = inverse
        stage_inv[...] = inverse

        @pl.when(me >= PLANE)
        def _():
            for z in range(1, planes - 1):
                remote(stage_inv, got_inv, send_inv, recv_inv, me + z * PLANE).start()
            late = jnp.logical_and(me == takers - 1, jnp.logical_not(zero_takes))
            to_first = remote(stage_inv, got_inv, send_first, recv_inv, 0)

            @pl.when(late)
            def _():
                to_first.start()
                to_first.wait_send()

            wait_rows(send_inv, planes - 2)

    @pl.when(jnp.logical_not(taker))
    def _():
        wait_rows(recv_inv, 1)
        inv_ref[...] = got_inv[...]


def scale(log_ref, inv_ref, out_hbm, scaled, sem):
    inverse = inv_ref[...]
    rows = log_ref.shape[1] // (PIECES // 3)
    copies = []
    for i in range(PIECES):
        d, at = i // (PIECES // 3), pl.ds(i % (PIECES // 3) * rows, rows)
        scaled[d, at, :] = log_ref[d, at, :] * inverse
        copy = pltpu.make_async_copy(scaled.at[d, at], out_hbm.at[d, at], sem.at[i])
        copy.start()
        copies.append(copy)
    for copy in copies:
        copy.wait()


def local(n, pressure, adjoint, permeability, active, fault_codes):
    steps, layers, rows, lanes = pressure.shape
    cells = layers * rows
    high = rows - LOW
    planes = n // PLANE
    vmem, dma = pltpu.VMEM, pltpu.SemaphoreType.DMA
    low_tile, high_tile = vmem((LOW, lanes), F32), vmem((high, lanes), F32)
    scratch = [
        vmem((2 * steps, cells + 8, lanes), F32),
        vmem((3, cells + 8, lanes), F32),
        vmem((cells + 8, lanes), jnp.int32),
        vmem((3, cells, lanes), jnp.int32),
        vmem((cells, lanes), F32),
        vmem((cells + 8, lanes), F32),
        vmem((2 * steps, LOW, lanes), F32), vmem((2, LOW, lanes), F32),
        vmem((2 * steps, high, lanes), F32), vmem((3, high, lanes), F32),
        vmem((2, LOW, lanes), F32), vmem((3, high, lanes), F32),
        low_tile, high_tile, low_tile, high_tile,
        vmem((1, lanes), F32), vmem((n, 1, lanes), F32),
        vmem((1, lanes), F32), vmem((1, lanes), F32),
        dma((6,)), dma, dma((2,)), dma, dma((2,)),
        dma((2,)), dma, dma, dma, dma,
    ]
    hbm = pl.BlockSpec(memory_space=pltpu.HBM)
    in_hbm = lambda x: pltpu.with_memory_space_constraint(x, pltpu.HBM)
    log, inverse = pl.pallas_call(
        functools.partial(kernel, steps, layers, rows, n),
        out_shape=(
            jax.ShapeDtypeStruct((3, cells, lanes), F32),
            jax.ShapeDtypeStruct((1, lanes), F32),
        ),
        in_specs=[hbm] * 5,
        out_specs=(pl.BlockSpec(memory_space=pltpu.VMEM), pl.BlockSpec(memory_space=pltpu.VMEM)),
        scratch_shapes=scratch,
        compiler_params=pltpu.CompilerParams(
            collective_id=0, has_side_effects=True, vmem_limit_bytes=32 * 1024 * 1024
        ),
        name="gradient",
    )(
        in_hbm(pressure.reshape(steps, cells, lanes)),
        in_hbm(adjoint.reshape(steps, cells, lanes)),
        in_hbm(permeability.reshape(3, cells, lanes)),
        in_hbm(active.reshape(cells, lanes)),
        in_hbm(fault_codes.reshape(3, cells, lanes)),
    )
    out = pl.pallas_call(
        scale,
        out_shape=jax.ShapeDtypeStruct(log.shape, F32),
        in_specs=[pl.BlockSpec(memory_space=pltpu.VMEM)] * 2,
        out_specs=pl.BlockSpec(memory_space=pltpu.HBM),
        scratch_shapes=[vmem(log.shape, F32), dma((PIECES,))],
        compiler_params=pltpu.CompilerParams(vmem_limit_bytes=8 * 1024 * 1024),
        name="scale",
    )(log, inverse)
    return out.reshape(3, layers, rows, lanes)


def solution(mesh):
    n = mesh.shape["gx"]
    whole = ("groups", "gx")
    four = P(None, whole, None, None)
    return jax.shard_map(
        functools.partial(local, n),
        mesh=mesh,
        in_specs=(four, four, four, P(whole, None, None), four),
        out_specs=four,
        check_vma=False,
    )
```

```python
import functools

import jax
import jax.numpy as jnp
from jax import lax
from jax.experimental import pallas as pl
from jax.experimental.pallas import tpu as pltpu
from jax.sharding import PartitionSpec as P

MESH = pl.DeviceIdType.MESH
F32 = jnp.float32

epsilon = 1e-06

PLANE = 8
BLOCK = 64

LOW = 56

PIECES = 6


def multiplier(codes):
    return jnp.where(codes == 0, 2.0, jnp.where(codes == 1, 1.2, jnp.where(codes == 2, 0.5, 0.1)))


def face(products, factor, lower_perm, upper_perm):
    inverse = 1.0 / (lower_perm + upper_perm)
    weight = factor * products
    upper = upper_perm * inverse
    lower = lower_perm * inverse
    return weight * upper * upper, weight * lower * lower


def kernel(
    steps, layers, rows, n,
    pres_hbm, adj_hbm, perm_hbm, act_hbm, code_hbm,
    log_ref, inv_ref,
    both, perm, act, code,
    to_up_x, to_up_y,
    above_both, above_rest, below_both, below_rest,
    stage_down, stage_up, stage_ra, stage_rb, got_ra, got_rb,
    stage_sum, sums, stage_inv, got_inv,
    load_sem, send_up, recv_up, send_down, recv_down,
    send_sum, recv_sum, send_inv, send_first, recv_inv, partner,
):
    high = rows - LOW

    def halves(ref):
        return ref.at[pl.ds(0, steps)], ref.at[pl.ds(steps, steps)]

    pres, adj = halves(both)
    above_pres, above_adj = halves(above_both)
    below_pres, below_adj = halves(below_both)
    above_perm, above_log = above_rest.at[0], above_rest.at[1]
    below_perm, below_factor, below_log = (below_rest.at[i] for i in range(3))
    cells = layers * rows
    top = cells - rows
    planes = n // PLANE
    takers = 2 * PLANE
    me = lax.axis_index("gx")
    first, last = me == 0, me == n - 1
    zero_takes = lax.axis_index("groups") != 0
    taker = jnp.logical_and(me < takers, jnp.logical_or(me > 0, zero_takes))
    up, down = me + 1, me - 1

    def wait_rows(sem, row_count, wide=1):
        ref = both.at[pl.ds(0, wide), pl.ds(0, row_count // wide)]
        pltpu.make_async_copy(ref, ref, sem).wait()

    def load(group, parts):
        for src, dst, begin, count in parts:
            at = pl.ds(begin, count)
            where = (at,) if len(src.shape) == 2 else (slice(None), at)
            pltpu.make_async_copy(src.at[where], dst.at[where], load_sem.at[group]).start()

    fields = [(pres_hbm, pres), (adj_hbm, adj)]
    others = [(perm_hbm, perm), (act_hbm, act), (code_hbm, code)]

    def span(refs, begin, end):
        return [(src, dst, begin, end - begin) for src, dst in refs]

    load(0, span(fields, top + LOW, cells))
    load(5, span(fields, 0, LOW))
    load(1, span(fields, LOW, 2 * rows) + span(others, 0, 2 * rows))

    barrier = pltpu.get_barrier_semaphore()

    def greet(device):
        pl.semaphore_signal(barrier, inc=1, device_id={"gx": device}, device_id_type=MESH)

    even = lax.rem(me, 2) == 0
    odd = jnp.logical_not(even)

    @pl.when(jnp.logical_not(last))
    def _():
        greet(up)

    @pl.when(jnp.logical_and(even, jnp.logical_not(first)))
    def _():
        greet(down)

    @pl.when(taker)
    def _():
        def body(device, carry):
            @pl.when(device != me)
            def _():
                greet(device)

            return carry

        lax.fori_loop(0, n, body, 0)

    zero8 = jnp.zeros((8, rows), F32)
    for t in range(steps):
        pres[t, pl.ds(cells, 8), :] = zero8
        adj[t, pl.ds(cells, 8), :] = zero8
    for d in range(3):
        perm[d, pl.ds(cells, 8), :] = zero8
    act[pl.ds(cells, 8), :] = jnp.zeros((8, rows), jnp.int32)
    to_up_y[pl.ds(0, 8), :] = zero8

    low_a = pl.ds(0, LOW)
    top_b = pl.ds(top + LOW, high)

    def remote(src, dst, send, recv, device):
        return pltpu.make_async_remote_copy(
            src_ref=src, dst_ref=dst, send_sem=send, recv_sem=recv,
            device_id={"gx": device}, device_id_type=MESH,
        )

    goes_down = [
        remote(s, d, send_down, recv_down.at[i], down)
        for i, (s, d) in enumerate([(both.at[:, low_a], above_both), (stage_down, above_rest), (stage_rb, got_rb)])
    ]
    goes_up = [
        remote(s, d, send_up, recv_up.at[i], up)
        for i, (s, d) in enumerate([(both.at[:, top_b], below_both), (stage_up, below_rest), (stage_ra, got_ra)])
    ]

    def start_up(*parts):
        @pl.when(jnp.logical_not(last))
        def _():
            for i in parts:
                goes_up[i].start()

    def start_down(*parts):
        @pl.when(jnp.logical_not(first))
        def _():
            for i in parts:
                goes_down[i].start()

    def one_if(condition):
        return jnp.where(condition, 1, 0)

    wait_rows(load_sem.at[0], 2 * steps * high, steps)
    pl.semaphore_wait(barrier, takers + one_if(odd) + one_if(zero_takes) - one_if(first) - one_if(last) - one_if(taker))
    @pl.when(odd)
    def _():
        pl.semaphore_signal(partner, inc=1, device_id={"gx": down}, device_id_type=MESH)
        start_up(0)

    wait_rows(load_sem.at[5], 2 * steps * LOW, steps)
    start_down(0)

    load(2, span(fields, 6 * rows, top + LOW) + span(others, 6 * rows, cells))

    @pl.when(even)
    def _():
        pl.semaphore_wait(partner, 1)
        start_up(0)

    first_two = 2 * steps * (2 * rows - LOW) + 7 * 2 * rows
    last_two = 2 * steps * (rows + LOW) + 7 * 2 * rows
    whole = (2 * steps + 7) * 2 * rows

    lane = lax.broadcasted_iota(jnp.int32, (BLOCK, rows), 1)
    sub = lax.broadcasted_iota(jnp.int32, (BLOCK, rows), 0)
    z_open = jnp.where(lane == rows - 1, 0.0, 1.0).astype(F32)

    def fold(square):
        return jnp.sum(square.reshape(square.shape[0] // 8, 8, rows), axis=0)

    def block(start, in_layer, acc, from_below, to_above):
        at = pl.ds(start, BLOCK)
        next_row = pl.ds(start + 1, BLOCK)
        next_layer = pl.ds(start + rows, BLOCK)
        px = py = pz = None
        for t in range(steps):
            p, a = pres[t, at, :], adj[t, at, :]
            y = (a - adj[t, next_row, :]) * (p - pres[t, next_row, :])
            z = (a - pltpu.roll(a, rows - 1, 1)) * (p - pltpu.roll(p, rows - 1, 1))
            py = y if t == 0 else py + y
            pz = z if t == 0 else pz + z
            if to_above:
                x = (a - adj[t, next_layer, :]) * (p - pres[t, next_layer, :])
                px = x if t == 0 else px + x
        opened = act[at, :].astype(F32)

        k = perm[2, at, :]
        factor = multiplier(code[2, at, :]) * opened * pltpu.roll(opened, rows - 1, 1) * z_open
        mine, above = face(pz, factor, k, pltpu.roll(k, rows - 1, 1))
        log = k * (mine + pltpu.roll(above, 1, 1))
        log_ref[2, at, :] = log
        acc = acc + fold(log * log)

        k = perm[1, at, :]
        y_open = jnp.where(in_layer + sub == rows - 1, 0.0, 1.0).astype(F32)
        factor = multiplier(code[1, at, :]) * opened * act[next_row, :].astype(F32) * y_open
        mine, above = face(py, factor, k, perm[1, next_row, :])
        to_up_y[next_row, :] = above
        log = k * (mine + to_up_y[at, :])
        log_ref[1, at, :] = log
        acc = acc + fold(log * log)

        k = perm[0, at, :]
        total = None
        if to_above:
            factor = multiplier(code[0, at, :]) * opened * act[next_layer, :].astype(F32)
            mine, above = face(px, factor, k, perm[0, next_layer, :])
            to_up_x[next_layer, :] = above
            total = mine
        if from_below:
            into = to_up_x[at, :]
            total = into if total is None else total + into
        log = k * total
        log_ref[0, at, :] = log
        if from_below and to_above:
            acc = acc + fold(log * log)
        return acc

    def layer_of(layer, acc, from_below=True, to_above=True):
        def body(i, acc):
            in_layer = pl.multiple_of(i * BLOCK, BLOCK)
            return block(pl.multiple_of(layer * rows + in_layer, BLOCK), in_layer, acc, from_below, to_above)

        return lax.fori_loop(0, rows // BLOCK, body, acc)

    def middle(begin, end, acc):
        return lax.fori_loop(begin, end, layer_of, acc)

    def products_of(lower_pres, lower_adj, lower_at, upper_pres, upper_adj, upper_at):
        total = None
        for t in range(steps):
            term = (lower_adj[t, lower_at, :] - upper_adj[t, upper_at, :]) * (
                lower_pres[t, lower_at, :] - upper_pres[t, upper_at, :]
            )
            total = term if t == 0 else total + term
        return total

    wait_rows(load_sem.at[1], first_two, steps)
    load(3, span(fields + others, 2 * rows, 4 * rows))
    stage_down[0] = perm[0, low_a, :] * act[low_a, :].astype(F32)
    acc = layer_of(0, jnp.zeros((8, rows), F32), from_below=False)
    stage_down[1] = log_ref[0, low_a, :]

    wait_rows(load_sem.at[2], last_two, steps)
    load(4, span(fields + others, 4 * rows, 6 * rows))
    start_down(1)
    stage_up[0] = perm[0, top_b, :]
    under = pl.ds(top - rows + LOW, high)
    products = products_of(pres, adj, under, pres, adj, top_b)
    opened = act[top_b, :].astype(F32)
    stage_up[1] = multiplier(code[0, top_b, :]) * opened
    factor = multiplier(code[0, under, :]) * act[under, :].astype(F32) * opened
    stage_up[2] = perm[0, top_b, :] * face(products, factor, perm[0, under, :], perm[0, top_b, :])[1]

    wait_rows(load_sem.at[3], whole, steps)
    acc = layer_of(1, acc)
    start_up(1)
    acc = layer_of(2, acc)
    wait_rows(load_sem.at[4], whole, steps)
    acc = middle(3, layers - 1, acc)
    acc = layer_of(layers - 1, acc, to_above=False)

    @pl.when(jnp.logical_not(last))
    def _():
        wait_rows(recv_down.at[0], 2 * steps * LOW, 2)

    def keep(condition, value):
        return jnp.where(condition, value, 0.0)

    everything, here = pl.ds(0, LOW), pl.ds(top, LOW)
    inside = jnp.logical_not(last)
    products = products_of(pres, adj, here, above_pres, above_adj, everything)

    @pl.when(jnp.logical_not(last))
    def _():
        wait_rows(recv_down.at[1], 2 * LOW, 2)

    factor = multiplier(code[0, here, :]) * act[here, :].astype(F32)
    k, k_up = perm[0, here, :], above_perm[...]
    mine, other = face(products, factor, k, k_up)
    log = log_ref[0, here, :] + keep(inside, k * mine)
    log_ref[0, here, :] = log
    reply = k_up * other
    stage_ra[...] = reply
    reply = keep(inside, reply + above_log[...])
    end = keep(last, log_ref[0, top_b, :])
    acc = acc + fold(log * log) + fold(reply * reply) + fold(end * end)

    @pl.when(jnp.logical_not(first))
    def _():
        wait_rows(recv_up.at[0], 2 * steps * high, 2)

    everything, here = pl.ds(0, high), pl.ds(LOW, high)
    inside = jnp.logical_not(first)
    products = products_of(below_pres, below_adj, everything, pres, adj, here)

    @pl.when(jnp.logical_not(first))
    def _():
        wait_rows(recv_up.at[1], 3 * high, 1)

    factor = below_factor[...] * act[here, :].astype(F32)
    k, k_low = perm[0, here, :], below_perm[...]
    other, mine = face(products, factor, k_low, k)
    log = log_ref[0, here, :] + keep(inside, k * mine)
    log_ref[0, here, :] = log
    reply = k_low * other
    stage_rb[...] = reply
    reply = keep(inside, reply + below_log[...])
    end = keep(first, log_ref[0, low_a, :])
    acc = acc + fold(log * log) + fold(reply * reply) + fold(end * end)

    partial = jnp.sum(acc, axis=0, keepdims=True)
    stage_sum[...] = partial
    to_takers = [remote(stage_sum, sums.at[me], send_sum.at[int(q == 0)], recv_sum, q) for q in range(takers)]
    to_zero = jnp.logical_and(zero_takes, jnp.logical_not(first))

    @pl.when(to_zero)
    def _():
        to_takers[0].start()

    @pl.when(jnp.logical_not(taker))
    def _():
        for copy in to_takers[1:]:
            copy.start()

    @pl.when(taker)
    def _():
        for q in range(1, takers):
            @pl.when(me != q)
            def _():
                to_takers[q].start()

    start_up(2)
    start_down(2)

    @pl.when(jnp.logical_not(first))
    def _():
        wait_rows(recv_up.at[2], LOW)
        log_ref[0, low_a, :] += got_ra[...]
        wait_rows(send_down, (2 * steps + 2) * LOW + high, 2)

    @pl.when(jnp.logical_not(last))
    def _():
        wait_rows(recv_down.at[2], high)
        log_ref[0, top_b, :] += got_rb[...]
        wait_rows(send_up, (2 * steps + 3) * high + LOW, 2)

    @pl.when(to_zero)
    def _():
        wait_rows(send_sum.at[1], 1)

    @pl.when(jnp.logical_and(taker, jnp.logical_not(first)))
    def _():
        wait_rows(send_sum.at[0], takers - 2)

    @pl.when(jnp.logical_or(first, jnp.logical_not(taker)))
    def _():
        wait_rows(send_sum.at[0], takers - 1)

    @pl.when(taker)
    def _():
        sums[me] = partial
        wait_rows(recv_sum, n - 1)
        quarter = n // 4
        total = sum(jnp.sum(sums[pl.ds(q * quarter, quarter)], axis=0) for q in range(4))
        total = jnp.sum(total, axis=1, keepdims=True)
        entries = 3 * cells * rows * n
        inverse = jnp.broadcast_to(1.0 / jnp.sqrt(total / entries + epsilon), inv_ref.shape)
        inv_ref[...] = inverse
        stage_inv[...] = inverse

        @pl.when(me >= PLANE)
        def _():
            for z in range(1, planes - 1):
                remote(stage_inv, got_inv, send_inv, recv_inv, me + z * PLANE).start()
            late = jnp.logical_and(me == takers - 1, jnp.logical_not(zero_takes))
            to_first = remote(stage_inv, got_inv, send_first, recv_inv, 0)

            @pl.when(late)
            def _():
                to_first.start()
                to_first.wait_send()

            wait_rows(send_inv, planes - 2)

    @pl.when(jnp.logical_not(taker))
    def _():
        wait_rows(recv_inv, 1)
        inv_ref[...] = got_inv[...]


def scale(log_ref, inv_ref, out_hbm, scaled, sem):
    inverse = inv_ref[...]
    rows = log_ref.shape[1] // (PIECES // 3)
    copies = []
    for i in range(PIECES):
        d, at = i // (PIECES // 3), pl.ds(i % (PIECES // 3) * rows, rows)
        scaled[d, at, :] = log_ref[d, at, :] * inverse
        copy = pltpu.make_async_copy(scaled.at[d, at], out_hbm.at[d, at], sem.at[i])
        copy.start()
        copies.append(copy)
    for copy in copies:
        copy.wait()


def local(n, pressure, adjoint, permeability, active, fault_codes):
    steps, layers, rows, lanes = pressure.shape
    cells = layers * rows
    high = rows - LOW
    planes = n // PLANE
    vmem, dma = pltpu.VMEM, pltpu.SemaphoreType.DMA
    low_tile, high_tile = vmem((LOW, lanes), F32), vmem((high, lanes), F32)
    scratch = [
        vmem((2 * steps, cells + 8, lanes), F32),
        vmem((3, cells + 8, lanes), F32),
        vmem((cells + 8, lanes), jnp.int32),
        vmem((3, cells, lanes), jnp.int32),
        vmem((cells, lanes), F32),
        vmem((cells + 8, lanes), F32),
        vmem((2 * steps, LOW, lanes), F32), vmem((2, LOW, lanes), F32),
        vmem((2 * steps, high, lanes), F32), vmem((3, high, lanes), F32),
        vmem((2, LOW, lanes), F32), vmem((3, high, lanes), F32),
        low_tile, high_tile, low_tile, high_tile,
        vmem((1, lanes), F32), vmem((n, 1, lanes), F32),
        vmem((1, lanes), F32), vmem((1, lanes), F32),
        dma((6,)), dma, dma((3,)), dma, dma((3,)),
        dma((2,)), dma, dma, dma, dma, pltpu.SemaphoreType.REGULAR,
    ]
    hbm = pl.BlockSpec(memory_space=pltpu.HBM)
    in_hbm = lambda x: pltpu.with_memory_space_constraint(x, pltpu.HBM)
    log, inverse = pl.pallas_call(
        functools.partial(kernel, steps, layers, rows, n),
        out_shape=(
            jax.ShapeDtypeStruct((3, cells, lanes), F32),
            jax.ShapeDtypeStruct((1, lanes), F32),
        ),
        in_specs=[hbm] * 5,
        out_specs=(pl.BlockSpec(memory_space=pltpu.VMEM), pl.BlockSpec(memory_space=pltpu.VMEM)),
        scratch_shapes=scratch,
        compiler_params=pltpu.CompilerParams(
            collective_id=0, has_side_effects=True, vmem_limit_bytes=32 * 1024 * 1024
        ),
        name="gradient",
    )(
        in_hbm(pressure.reshape(steps, cells, lanes)),
        in_hbm(adjoint.reshape(steps, cells, lanes)),
        in_hbm(permeability.reshape(3, cells, lanes)),
        in_hbm(active.reshape(cells, lanes)),
        in_hbm(fault_codes.reshape(3, cells, lanes)),
    )
    out = pl.pallas_call(
        scale,
        out_shape=jax.ShapeDtypeStruct(log.shape, F32),
        in_specs=[pl.BlockSpec(memory_space=pltpu.VMEM)] * 2,
        out_specs=pl.BlockSpec(memory_space=pltpu.HBM),
        scratch_shapes=[vmem(log.shape, F32), dma((PIECES,))],
        compiler_params=pltpu.CompilerParams(vmem_limit_bytes=8 * 1024 * 1024),
        name="scale",
    )(log, inverse)
    return out.reshape(3, layers, rows, lanes)


def solution(mesh):
    n = mesh.shape["gx"]
    whole = ("groups", "gx")
    four = P(None, whole, None, None)
    return jax.shard_map(
        functools.partial(local, n),
        mesh=mesh,
        in_specs=(four, four, four, P(whole, None, None), four),
        out_specs=four,
        check_vma=False,
    )
```
